32 devices in a mesh: depth: 4 (over y, core), blk: 8 (over z, x).
Axes of the slice: x: 2, y: 2, z: 4, core: 2. Of those that a mesh axis runs over, the one named last changes fastest.
Arguments:
- jacobian: bfloat16 [96, 16384], P(('depth', 'blk')), may hold values from -6 to 6
- gain_inverse: bfloat16 [16384, 16384], P('depth', 'blk'), may hold values from -0.00024414062 to 0.00048828125, as said below
- variance: float32 [96], P(('depth', 'blk')), may hold values from 2 to 12
Outputs:
- omega_diag: float32 [96], P(('depth', 'blk'))
The draws below stay inside these ranges and needn't reach their ends.
Inputs may be any that keep to these rules, and one draw needn't show every extreme that they name: gain_inverse is symmetric and positive definite.
All inputs are finite; a program needn't handle non-finite values.
Results may differ from the reference program's by a relative error of at most 0.0003.
Values may be sent and summed in bfloat16 or wider, within the bound.
A program may use at most 128 MiB of HBM per device.

```python
import math
import jax
import jax.numpy as jnp

S = 16384
M = 96


def draw_gain_inverse(key, part):
    noise_key = jax.random.fold_in(key, 11)
    gains_key = jax.random.fold_in(key, 23)
    gains = jnp.exp(jax.random.uniform(gains_key, (S,), jnp.float32, jnp.log(0.6), jnp.log(1.6)))
    noise = jax.random.normal(noise_key, (S, S), jnp.float32)
    places = jnp.arange(S).astype(jnp.float32)
    distance = jnp.abs(places[:, None] - places[None, :])
    kernel = jnp.exp(-distance / (S / 4.0))
    ident = (distance == 0.0).astype(jnp.float32)
    rough = (noise + noise.T) * (0.4 / jnp.sqrt(2.0 * S))
    matrix = gains[:, None] * gains[None, :] * (ident + kernel + rough) / (2.0 * S)
    return matrix.astype(jnp.bfloat16)


def block_levels(own_key, dims, split, low, top_value):
    factor_of, own = 1.0, jax.random.fold_in(own_key, 6)
    for axis_at, parts in split:
        heights = jnp.exp(jax.random.uniform(jax.random.fold_in(own, axis_at), (parts,), jnp.float32, low / len(split), top_value / len(split)))
        factor_of = factor_of * jnp.repeat(heights, dims[axis_at] // parts).reshape([-1 if axis == axis_at else 1 for axis in range(len(dims))])
    return factor_of


def bell_draw(rng, extent, scale, reach, split=(), kind=jnp.bfloat16):
    drawn = jax.random.normal(rng, extent, jnp.float32) * scale
    if len(split) > 0:
        drawn = block_levels(rng, extent, split, -0.22, 0.18) * drawn
    return jnp.clip(drawn, min=-reach, max=reach).astype(kind)


def setup_inputs(seed: int = 0) -> dict:
    seeds = jax.random.split(jax.random.key(seed), 4)
    jacobian = bell_draw(seeds[0], (M, S), 1.0, 6.0, ((0, 32),))
    gain_inverse = draw_gain_inverse(jax.random.fold_in(seeds[3], 71), 0)
    variance = jnp.clip(jnp.exp(math.log(12.0) - 1.7917595 * jax.random.uniform(seeds[2], (M,), jnp.float32) ** block_levels(seeds[2], (M,), ((0, 32),), -0.2, 0.2)), 2.0, 12.0)
    return {"jacobian": jacobian, "gain_inverse": gain_inverse, "variance": variance}


def reference(jacobian, gain_inverse, variance):
    projected = jnp.dot(jacobian, gain_inverse, preferred_element_type=jnp.float32)
    quadratic = jnp.sum(projected * jacobian.astype(jnp.float32), axis=1)
    return variance - quadratic
```

```python
import functools

import jax
import jax.numpy as jnp
from jax import lax
from jax.experimental import pallas as pl
from jax.experimental.pallas import tpu as pltpu
from jax.sharding import PartitionSpec as P

LANES = 128
SUBLANES = 8
PACKED = 16
MESH = pl.DeviceIdType.MESH


def exchange_kernel(depth_count, blk_count, slots, *refs):
    count = len(slots)
    sources, targets = refs[:count], refs[count : 2 * count]
    send_sem, recv_sem, own_sem = refs[2 * count :]
    devices = depth_count * blk_count
    me = lax.axis_index("depth") * blk_count + lax.axis_index("blk")

    def place(device):
        return {"depth": device // blk_count, "blk": lax.rem(device, blk_count)}

    def peer(step):
        return lax.rem(me + step, devices)

    def slot_of(kind, device):
        if kind == "depth":
            return device // blk_count
        if kind == "blk":
            return lax.rem(device, blk_count)
        return device

    def copy(which, step):
        device = peer(step)
        return pltpu.make_async_remote_copy(
            src_ref=sources[which].at[slot_of(slots[which], device)],
            dst_ref=targets[which].at[me],
            send_sem=send_sem.at[which, step],
            recv_sem=recv_sem.at[which, step],
            device_id=place(device),
            device_id_type=MESH,
        )

    barrier = pltpu.get_barrier_semaphore()

    @pl.loop(1, devices)
    def _(step):
        pl.semaphore_signal(barrier, inc=1, device_id=place(peer(step)), device_id_type=MESH)

    own = [
        pltpu.make_async_copy(sources[w].at[slot_of(slots[w], me)], targets[w].at[me], own_sem.at[w])
        for w in range(count)
    ]
    for w in range(count):
        own[w].start()
    pl.semaphore_wait(barrier, devices - 1)

    @pl.loop(1, devices)
    def _(step):
        for w in range(count):
            copy(w, step).start()

    for w in range(count):
        own[w].wait()

    @pl.loop(1, devices)
    def _(step):
        for w in range(count):
            copy(w, step).wait()


def exchange(slots, collective_id, *operands):
    depth_count = lax.axis_size("depth")
    blk_count = lax.axis_size("blk")
    devices = depth_count * blk_count
    count = len(slots)
    vmem = pl.BlockSpec(memory_space=pltpu.VMEM)
    return pl.pallas_call(
        functools.partial(exchange_kernel, depth_count, blk_count, slots),
        out_shape=[jax.ShapeDtypeStruct((devices,) + x.shape[1:], x.dtype) for x in operands],
        in_specs=[vmem] * count,
        out_specs=[vmem] * count,
        scratch_shapes=[
            pltpu.SemaphoreType.DMA((count, devices)),
            pltpu.SemaphoreType.DMA((count, devices)),
            pltpu.SemaphoreType.DMA((count,)),
        ],
        compiler_params=pltpu.CompilerParams(collective_id=collective_id, has_side_effects=True),
    )(*operands)


def sections(jacobian, parts):
    rows, states = jacobian.shape
    width = states // parts
    return jacobian.reshape(rows, parts, width // LANES, LANES).transpose(1, 0, 2, 3)


def plain_shards(jacobian, gain_inverse, variance):
    rows = jacobian.shape[0]
    depth_count = lax.axis_size("depth")
    blk_count = lax.axis_size("blk")
    devices = depth_count * blk_count
    left, right = exchange(
        ("depth", "blk"), 0, sections(jacobian, depth_count), sections(jacobian, blk_count)
    )
    left = left.reshape(devices * rows, -1)
    panel = right.reshape(devices * rows, -1)
    projected = jnp.dot(left, gain_inverse, preferred_element_type=jnp.float32)
    partial_sum = jnp.sum(projected * panel.astype(jnp.float32), axis=1)
    padded = jnp.pad(
        partial_sum.reshape(devices, 1, rows), ((0, 0), (0, SUBLANES - 1), (0, LANES - rows))
    )
    (gathered,) = exchange(("all",), 1, padded)
    quadratic = jnp.sum(gathered[:, 0, :rows], axis=0)
    return variance - quadratic


def half_kernel(
    depth_count, blk_count, rows, jac_ref, gain_ref, out_ref,
    own_raw, own_wide, lines, other_in, panel_in, other_out, panel_out, wide,
    gain, left, parts, arrived,
    local_sem, chain_send, chain_recv, plane_send, plane_recv, last_send, last_recv,
):
    per = blk_count // depth_count
    planes = depth_count
    group = depth_count * per
    devices = depth_count * blk_count
    states = jac_ref.shape[1]
    chunks = states // LANES
    sub = states // blk_count // LANES
    width = sub * LANES
    pitch = rows * sub + 1
    depth = lax.axis_index("depth")
    blk = lax.axis_index("blk")
    plane = blk // per
    side = lax.rem(blk, per)
    spot = depth * per + side
    on_diagonal = plane == depth

    def other_half(d, z, s):
        return jnp.where(d < z, s, per - 1 - s)

    def other_section(d, z, s):
        return d * per + other_half(d, z, s)

    def peer(step):
        return lax.rem(spot + step, group)

    def place(member, z):
        return {"depth": member // per, "blk": z * per + lax.rem(member, per)}

    half = other_half(depth, plane, side)
    jac_copy = pltpu.make_async_copy(jac_ref, own_raw, local_sem.at[0])
    jac_copy.start()
    gain_other = pltpu.make_async_copy(
        gain_ref.at[pl.ds(pl.multiple_of(half * width, width), width), :], gain.at[0], local_sem.at[1]
    )
    gain_own = pltpu.make_async_copy(
        gain_ref.at[pl.ds(pl.multiple_of(side * width, width), width), :], gain.at[1], local_sem.at[2]
    )
    gain_other.start()

    @pl.when(on_diagonal)
    def _():
        gain_own.start()

    barrier = pltpu.get_barrier_semaphore()

    @pl.loop(1, devices)
    def _(step):
        target = lax.rem(depth * blk_count + blk + step, devices)
        pl.semaphore_signal(
            barrier, inc=1,
            device_id={"depth": target // blk_count, "blk": lax.rem(target, blk_count)},
            device_id_type=MESH,
        )

    jac_copy.wait()
    for c in range(chunks):
        own_wide[pl.ds(c, rows, stride=chunks), :] = own_raw[:, c * LANES : (c + 1) * LANES].astype(
            jnp.float32
        )
    for r in range(rows):
        lines[plane, r] = own_wide[r * chunks : (r + 1) * chunks, :].astype(jnp.bfloat16)

    pl.semaphore_wait(barrier, devices - 1)

    def chain(source, target, way):
        return pltpu.make_async_remote_copy(
            src_ref=lines.at[source],
            dst_ref=lines.at[source],
            send_sem=chain_send.at[source, way],
            recv_sem=chain_recv.at[source],
            device_id={"depth": depth, "blk": target * per + side},
            device_id_type=MESH,
        )

    def section_of(source, section):
        return lines.at[source, :, pl.ds(pl.multiple_of(section * sub, sub), sub), :]

    def to_other(source, step):
        member = peer(step)
        section = other_section(member // per, plane, lax.rem(member, per))
        return pltpu.make_async_remote_copy(
            src_ref=section_of(source, section),
            dst_ref=other_in.at[source, spot],
            send_sem=plane_send.at[0, source, step],
            recv_sem=plane_recv.at[0, source, spot],
            device_id=place(member, plane),
            device_id_type=MESH,
        )

    def to_panel(source, step):
        member = peer(step)
        return pltpu.make_async_remote_copy(
            src_ref=section_of(source, plane * per + lax.rem(member, per)),
            dst_ref=panel_in.at[source, spot],
            send_sem=plane_send.at[1, source, step],
            recv_sem=plane_recv.at[1, source, spot],
            device_id=place(member, plane),
            device_id_type=MESH,
        )

    def spread(source):
        @pl.loop(1, group)
        def _(step):
            to_other(source, step).start()
            to_panel(source, step).start()

    def stages(act):
        for distance in range(1, planes):
            below = plane - distance
            above = plane + distance

            @pl.when(below >= 0)
            def _():
                act(below, plane + 1, 0)

            @pl.when(above < planes)
            def _():
                act(above, plane - 1, 1)

    @pl.when(plane + 1 < planes)
    def _():
        chain(plane, plane + 1, 0).start()

    @pl.when(plane > 0)
    def _():
        chain(plane, plane - 1, 1).start()

    spread(plane)

    def pass_on(source, onward, way):
        chain(source, source, way).wait_recv()

        @pl.when((onward < planes) & (onward >= 0))
        def _():
            chain(source, onward, way).start()

        spread(source)

    stages(pass_on)

    my_other = other_section(depth, plane, side)

    def widen(index, slot, block):
        wide[index, pl.ds(slot * pitch, rows * sub), :] = block.reshape(rows * sub, LANES).astype(
            jnp.float32
        )

    def slot_of(source, member):
        return (member // per) * blk_count + source * per + lax.rem(member, per)

    def collect(source):
        widen(0, slot_of(source, spot), section_of(source, my_other)[...])
        widen(1, slot_of(source, spot), section_of(source, blk)[...])

        @pl.loop(1, group)
        def _(step):
            member = peer(step)
            slot = slot_of(source, member)
            for which, buffer in enumerate((other_in, panel_in)):
                pltpu.make_async_copy(
                    buffer.at[source, member], buffer.at[source, member], plane_recv.at[which, source, member]
                ).wait()
                widen(which, slot, buffer[source, member])

    collect(plane)
    stages(lambda source, onward, way: collect(source))

    def columns(index, c):
        return [
            wide[index, pl.ds(r * sub + c, devices, stride=pitch), :] for r in range(rows)
        ]

    for c in range(sub):
        for r, block in enumerate(columns(0, c)):
            left[0, r * devices : (r + 1) * devices, c * LANES : (c + 1) * LANES] = block.astype(
                jnp.bfloat16
            )

    block_width = 4 * LANES

    def quadratic(index):
        total = [jnp.zeros((devices, LANES), jnp.float32) for _ in range(rows)]
        for n in range(width // block_width):
            product = jnp.dot(
                left[index], gain[index, :, n * block_width : (n + 1) * block_width],
                preferred_element_type=jnp.float32,
            )
            for c in range(block_width // LANES):
                panel = columns(1, n * (block_width // LANES) + c)
                for r in range(rows):
                    total[r] += (
                        product[r * devices : (r + 1) * devices, c * LANES : (c + 1) * LANES] * panel[r]
                    )
        return total

    gain_other.wait()
    weight = jnp.where(on_diagonal, 1.0, 2.0)
    for r, part in enumerate(quadratic(0)):
        parts[r] = part * weight

    @pl.when(on_diagonal)
    def _():
        for c in range(sub):
            for r, block in enumerate(columns(1, c)):
                left[1, r * devices : (r + 1) * devices, c * LANES : (c + 1) * LANES] = block.astype(
                    jnp.bfloat16
                )
        gain_own.wait()
        for r, part in enumerate(quadratic(1)):
            parts[r] += part

    lane = lax.broadcasted_iota(jnp.int32, (devices, LANES), 1)
    packed = jnp.zeros((devices, LANES), jnp.float32)
    for r in range(rows):
        packed = jnp.where(lane == r, jnp.sum(parts[r], axis=1, keepdims=True), packed)
    for t in range(devices):
        arrived[devices + t] = packed[t : t + 1]

    me = depth * blk_count + blk

    def last(step):
        target = lax.rem(me + step, devices)
        return pltpu.make_async_remote_copy(
            src_ref=arrived.at[devices + target],
            dst_ref=arrived.at[me],
            send_sem=last_send.at[step],
            recv_sem=last_recv.at[step],
            device_id={"depth": target // blk_count, "blk": lax.rem(target, blk_count)},
            device_id_type=MESH,
        )

    @pl.loop(1, devices)
    def _(step):
        last(step).start()

    arrived[me] = arrived[devices + me]

    def sent(source, onward, way):
        @pl.when((onward < planes) & (onward >= 0))
        def _():
            chain(source, onward, way).wait_send()

        @pl.loop(1, group)
        def _(step):
            to_other(source, step).wait_send()
            to_panel(source, step).wait_send()

    @pl.when(plane + 1 < planes)
    def _():
        chain(plane, plane + 1, 0).wait_send()

    @pl.when(plane > 0)
    def _():
        chain(plane, plane - 1, 1).wait_send()

    @pl.loop(1, group)
    def _(step):
        to_other(plane, step).wait_send()
        to_panel(plane, step).wait_send()

    stages(sent)

    @pl.loop(1, devices)
    def _(step):
        last(step).wait()

    total = arrived[0]
    for t in range(1, devices):
        total += arrived[t]
    out_ref[...] = total


def half_shards(jacobian, gain_inverse, variance):
    rows, states = jacobian.shape
    depth_count = lax.axis_size("depth")
    blk_count = lax.axis_size("blk")
    devices = depth_count * blk_count
    per = blk_count // depth_count
    planes, group = depth_count, depth_count * per
    chunks = states // LANES
    sub = states // blk_count // LANES
    width = sub * LANES
    bf16, f32 = jnp.bfloat16, jnp.float32
    dma = pltpu.SemaphoreType.DMA
    quadratic = pl.pallas_call(
        functools.partial(half_kernel, depth_count, blk_count, rows),
        out_shape=jax.ShapeDtypeStruct((1, LANES), f32),
        in_specs=[pl.BlockSpec(memory_space=pl.ANY)] * 2,
        out_specs=pl.BlockSpec(memory_space=pltpu.VMEM),
        scratch_shapes=[
            pltpu.VMEM((rows, states), bf16),
            pltpu.VMEM((rows * chunks, LANES), f32),
            pltpu.VMEM((planes, rows, chunks, LANES), bf16),
            pltpu.VMEM((planes, group, rows, sub, LANES), bf16),
            pltpu.VMEM((planes, group, rows, sub, LANES), bf16),
            pltpu.VMEM((SUBLANES, LANES), bf16),
            pltpu.VMEM((SUBLANES, LANES), bf16),
            pltpu.VMEM((2, devices * (rows * sub + 1), LANES), f32),
            pltpu.VMEM((2, width, width), bf16),
            pltpu.VMEM((2, rows * devices, width), bf16),
            pltpu.VMEM((rows, devices, LANES), f32),
            pltpu.VMEM((2 * devices, 1, LANES), f32),
            dma((3,)),
            dma((planes, 2)),
            dma((planes,)),
            dma((2, planes, group)),
            dma((2, planes, group)),
            dma((devices,)),
            dma((devices,)),
        ],
        compiler_params=pltpu.CompilerParams(
            collective_id=0, has_side_effects=True, vmem_limit_bytes=60 * 1024 * 1024
        ),
    )(jacobian, gain_inverse)
    return variance - quadratic[0, :rows]


def solution(mesh):
    in_specs = (P(("depth", "blk"), None), P("depth", "blk"), P(("depth", "blk")))
    out_specs = P(("depth", "blk"))
    depth_count, blk_count = mesh.shape["depth"], mesh.shape["blk"]

    def shards(jacobian, gain_inverse, variance):
        width = gain_inverse.shape[1]
        fits = gain_inverse.size * gain_inverse.dtype.itemsize <= 16 * 1024 * 1024
        if blk_count == 2 * depth_count and width % (PACKED * LANES) == 0 and fits:
            return half_shards(jacobian, gain_inverse, variance)
        return plain_shards(jacobian, gain_inverse, variance)

    return jax.shard_map(shards, mesh=mesh, in_specs=in_specs, out_specs=out_specs, check_vma=False)
```

```python
import functools

import jax
import jax.numpy as jnp
from jax import lax
from jax.experimental import pallas as pl
from jax.experimental.pallas import tpu as pltpu
from jax.sharding import PartitionSpec as P

LANES = 128
SUBLANES = 8
PACKED = 16
MESH = pl.DeviceIdType.MESH


def exchange_kernel(depth_count, blk_count, slots, *refs):
    count = len(slots)
    sources, targets = refs[:count], refs[count : 2 * count]
    send_sem, recv_sem, own_sem = refs[2 * count :]
    devices = depth_count * blk_count
    me = lax.axis_index("depth") * blk_count + lax.axis_index("blk")

    def place(device):
        return {"depth": device // blk_count, "blk": lax.rem(device, blk_count)}

    def peer(step):
        return lax.rem(me + step, devices)

    def slot_of(kind, device):
        if kind == "depth":
            return device // blk_count
        if kind == "blk":
            return lax.rem(device, blk_count)
        return device

    def copy(which, step):
        device = peer(step)
        return pltpu.make_async_remote_copy(
            src_ref=sources[which].at[slot_of(slots[which], device)],
            dst_ref=targets[which].at[me],
            send_sem=send_sem.at[which, step],
            recv_sem=recv_sem.at[which, step],
            device_id=place(device),
            device_id_type=MESH,
        )

    barrier = pltpu.get_barrier_semaphore()

    @pl.loop(1, devices)
    def _(step):
        pl.semaphore_signal(barrier, inc=1, device_id=place(peer(step)), device_id_type=MESH)

    own = [
        pltpu.make_async_copy(sources[w].at[slot_of(slots[w], me)], targets[w].at[me], own_sem.at[w])
        for w in range(count)
    ]
    for w in range(count):
        own[w].start()
    pl.semaphore_wait(barrier, devices - 1)

    @pl.loop(1, devices)
    def _(step):
        for w in range(count):
            copy(w, step).start()

    for w in range(count):
        own[w].wait()

    @pl.loop(1, devices)
    def _(step):
        for w in range(count):
            copy(w, step).wait()


def exchange(slots, collective_id, *operands):
    depth_count = lax.axis_size("depth")
    blk_count = lax.axis_size("blk")
    devices = depth_count * blk_count
    count = len(slots)
    vmem = pl.BlockSpec(memory_space=pltpu.VMEM)
    return pl.pallas_call(
        functools.partial(exchange_kernel, depth_count, blk_count, slots),
        out_shape=[jax.ShapeDtypeStruct((devices,) + x.shape[1:], x.dtype) for x in operands],
        in_specs=[vmem] * count,
        out_specs=[vmem] * count,
        scratch_shapes=[
            pltpu.SemaphoreType.DMA((count, devices)),
            pltpu.SemaphoreType.DMA((count, devices)),
            pltpu.SemaphoreType.DMA((count,)),
        ],
        compiler_params=pltpu.CompilerParams(collective_id=collective_id, has_side_effects=True),
    )(*operands)


def sections(jacobian, parts):
    rows, states = jacobian.shape
    width = states // parts
    return jacobian.reshape(rows, parts, width // LANES, LANES).transpose(1, 0, 2, 3)


def plain_shards(jacobian, gain_inverse, variance):
    rows = jacobian.shape[0]
    depth_count = lax.axis_size("depth")
    blk_count = lax.axis_size("blk")
    devices = depth_count * blk_count
    left, right = exchange(
        ("depth", "blk"), 0, sections(jacobian, depth_count), sections(jacobian, blk_count)
    )
    left = left.reshape(devices * rows, -1)
    panel = right.reshape(devices * rows, -1)
    projected = jnp.dot(left, gain_inverse, preferred_element_type=jnp.float32)
    partial_sum = jnp.sum(projected * panel.astype(jnp.float32), axis=1)
    padded = jnp.pad(
        partial_sum.reshape(devices, 1, rows), ((0, 0), (0, SUBLANES - 1), (0, LANES - rows))
    )
    (gathered,) = exchange(("all",), 1, padded)
    quadratic = jnp.sum(gathered[:, 0, :rows], axis=0)
    return variance - quadratic


def half_kernel(
    depth_count, blk_count, rows, jac_ref, gain_ref, out_ref,
    own_raw, own_wide, lines, other_in, panel_in, wide, gain, left, parts, outgoing, arrived,
    local_sem, line_send, line_recv, other_send, other_recv,
    panel_send, panel_recv, twin_send, twin_recv, last_send, last_recv, through_sem,
):
    per = blk_count // depth_count
    planes = depth_count
    group = depth_count * per
    half_group = group // 2
    devices = depth_count * blk_count
    states = jac_ref.shape[1]
    chunks = states // LANES
    sub = states // blk_count // LANES
    width = sub * LANES
    pitch = rows * sub + 1
    end = planes - 1
    depth = lax.axis_index("depth")
    blk = lax.axis_index("blk")
    plane = blk // per
    side = lax.rem(blk, per)
    spot = depth * per + side
    parity = lax.rem(depth, 2)
    twin = depth + 1 - 2 * parity
    seat = (depth // 2) * per + side
    on_diagonal = plane == depth

    def inside(z):
        return (z > 0) & (z < end)

    two_up = inside(plane + 2)
    two_down = inside(plane - 2)

    def wrap(value, count):
        return jnp.where(value >= count, value - count, value)

    def other_section(d, z, s):
        return d * per + jnp.where(d < z, s, per - 1 - s)

    my_other = other_section(depth, plane, side)

    def section_of(source, section):
        return lines.at[source, :, pl.ds(pl.multiple_of(section * sub, sub), sub), :]

    def remote(src, dst, send_sem, recv_sem, d, b):
        return pltpu.make_async_remote_copy(
            src_ref=src, dst_ref=dst, send_sem=send_sem, recv_sem=recv_sem,
            device_id={"depth": d, "blk": b}, device_id_type=MESH,
        )

    def settle(ref, sem):
        pltpu.make_async_copy(ref, ref, sem).wait()

    jac_copy = pltpu.make_async_copy(jac_ref, own_raw, local_sem.at[0])
    jac_copy.start()
    gain_other = pltpu.make_async_copy(
        gain_ref.at[pl.ds(pl.multiple_of((my_other - depth * per) * width, width), width), :],
        gain.at[0], local_sem.at[1],
    )
    gain_own = pltpu.make_async_copy(
        gain_ref.at[pl.ds(pl.multiple_of(side * width, width), width), :], gain.at[1], local_sem.at[2]
    )
    gain_other.start()

    @pl.when(on_diagonal)
    def _():
        gain_own.start()

    barrier = pltpu.get_barrier_semaphore()

    def greet(d, b):
        pl.semaphore_signal(barrier, inc=1, device_id={"depth": d, "blk": b}, device_id_type=MESH)

    @pl.when(plane < end)
    def _():
        greet(depth, blk + per)

    @pl.when(inside(plane) & (plane + 2 <= end))
    def _():
        greet(depth, blk + 2 * per)

    for s in range(1, group):
        member = wrap(spot + s, group)
        greet(member // per, plane * per + lax.rem(member, per))

    jac_copy.wait()
    for c in range(chunks):
        own_wide[pl.ds(c, rows, stride=chunks), :] = own_raw[:, c * LANES : (c + 1) * LANES].astype(
            jnp.float32
        )
    for r in range(rows):
        lines[plane, r] = own_wide[r * chunks : (r + 1) * chunks, :].astype(jnp.bfloat16)

    below = jnp.where(plane > 0, 1, 0) + jnp.where(two_down, 1, 0)
    pl.semaphore_wait(barrier, group - 1 + below)

    def along(source, part, target, send_sem):
        piece = lines.at[source, :, pl.ds(pl.multiple_of(part * (per * sub), per * sub), per * sub), :]
        return remote(piece, piece, send_sem, line_recv.at[source, part], depth, target * per + side)

    def first_part(source, target):
        relayed = jnp.where(
            (target == 0) & (source > 1), 1, jnp.where((target == end) & (source < end - 1), end - 1, target)
        )
        return wrap(relayed, planes)

    def send_line(target, sem_at):
        @pl.loop(0, planes)
        def _(k):
            part = wrap(first_part(plane, target) + k, planes)
            along(plane, part, target, line_send.at[sem_at]).start()

    def to_other(source, d, s):
        receiver = d * per + s
        seen = spot - receiver
        seen = jnp.where(seen < 0, seen + group, seen)
        return remote(
            section_of(source, other_section(d, plane, s)), other_in.at[source, seen],
            other_send.at[0], other_recv.at[source], d, plane * per + s,
        )

    def to_panel(source, step):
        target = wrap(seat + step, half_group)
        s = lax.rem(target, per)
        return remote(
            section_of(source, plane * per + s), panel_in.at[source, 0, half_group - step],
            panel_send.at[0], panel_recv.at[source], (target // per) * 2 + parity, plane * per + s,
        )

    def own_to_twin(source):
        return remote(
            section_of(source, blk), panel_in.at[source, 1, 0],
            twin_send.at[0], twin_recv.at[source], twin, blk,
        )

    def pass_to_twin(source):
        return remote(
            panel_in.at[source, 0, pl.ds(1, half_group - 1)], panel_in.at[source, 1, pl.ds(1, half_group - 1)],
            twin_send.at[0], twin_recv.at[source], twin, blk,
        )

    def spread(source, part):
        @pl.when(part == plane)
        def _():
            for step in range(1, half_group):
                to_panel(source, step).start()
            own_to_twin(source).start()

        for s in range(per):
            @pl.when((part != depth) | (side != s))
            def _():
                to_other(source, part, s).start()

    def forward_panel(source):
        settle(panel_in.at[source, 0, pl.ds(1, half_group - 1)], panel_recv.at[source])
        pass_to_twin(source).start()

    def tell(kind, b):
        pl.semaphore_signal(
            through_sem.at[kind], inc=1, device_id={"depth": depth, "blk": b}, device_id_type=MESH
        )

    @pl.when(plane > 0)
    def _():
        tell(0, blk - per)

    @pl.when(two_down)
    def _():
        send_line(plane - 2, 1)

    @pl.when(plane > 0)
    def _():
        send_line(plane - 1, 3)

    @pl.loop(0, planes)
    def _(k):
        spread(plane, wrap(plane + k, planes))

    @pl.when(plane < end)
    def _():
        pl.semaphore_wait(through_sem.at[0], 1)

    @pl.when((plane > 0) & inside(plane + 1))
    def _():
        tell(1, blk - per)

    @pl.when(two_up)
    def _():
        pl.semaphore_wait(through_sem.at[1], 1)
        send_line(plane + 2, 0)

    @pl.when(plane < end)
    def _():
        send_line(plane + 1, 2)

    def relays(source):
        down = (plane == 1) & (source > 1)
        up = (plane == end - 1) & (source < end - 1)
        return down, up

    def stages(act):
        for distance in range(1, planes):
            @pl.when(plane - distance >= 0)
            def _():
                act(plane - distance)

            @pl.when(plane + distance < planes)
            def _():
                act(plane + distance)

    def receive(source):
        down, up = relays(source)

        @pl.loop(0, planes)
        def _(k):
            part = wrap(first_part(source, plane) + k, planes)
            along(source, part, plane, line_send.at[0]).wait_recv()

            @pl.when(down | up)
            def _():
                along(source, part, jnp.where(down, 0, end), line_send.at[4 + source]).start()

            spread(source, part)

    stages(receive)
    forward_panel(plane)
    stages(forward_panel)

    def widen(index, slot, block):
        wide[index, pl.ds(slot * pitch, rows * sub), :] = block.reshape(rows * sub, LANES).astype(
            jnp.float32
        )

    def slot_of(source, d, s):
        return d * blk_count + source * per + s

    def collect(source):
        slot = slot_of(source, depth, side)
        widen(0, slot, section_of(source, my_other)[...])
        widen(1, slot, section_of(source, blk)[...])

        @pl.loop(1, half_group)
        def _(k):
            at = wrap(seat + k, half_group)
            widen(1, slot_of(source, (at // per) * 2 + parity, lax.rem(at, per)), panel_in[source, 0, k])

        settle(other_in.at[source, pl.ds(1, group - 1)], other_recv.at[source])

        @pl.loop(1, group)
        def _(k):
            member = wrap(spot + k, group)
            widen(0, slot_of(source, member // per, lax.rem(member, per)), other_in[source, k])

        settle(panel_in.at[source, 1], twin_recv.at[source])

        @pl.loop(0, half_group)
        def _(k):
            at = wrap(seat + k, half_group)
            widen(1, slot_of(source, (at // per) * 2 + 1 - parity, lax.rem(at, per)), panel_in[source, 1, k])

    collect(plane)
    stages(collect)

    def columns(index, c):
        return [wide[index, pl.ds(r * sub + c, devices, stride=pitch), :] for r in range(rows)]

    def narrow(index):
        for c in range(sub):
            for r, block in enumerate(columns(index, c)):
                left[index, r * devices : (r + 1) * devices, c * LANES : (c + 1) * LANES] = block.astype(
                    jnp.bfloat16
                )

    narrow(0)
    block_width = width // 4
    blocks = width // block_width
    inner = block_width // LANES

    def times_panel(total, product, n):
        for c in range(inner):
            panel = columns(1, n * inner + c)
            for r in range(rows):
                total[r] += product[r * devices : (r + 1) * devices, c * LANES : (c + 1) * LANES] * panel[r]

    def dot(index, first, count, n):
        if isinstance(first, int):
            a = left[index, :, first : first + count]
        else:
            a = left[index, :, pl.ds(pl.multiple_of(first, LANES), count)]
        b = gain[index, pl.ds(first, count), n * block_width : (n + 1) * block_width]
        return jnp.dot(a, b, preferred_element_type=jnp.float32)

    def zeros():
        return [jnp.zeros((devices, LANES), jnp.float32) for _ in range(rows)]

    gain_other.wait()

    @pl.when(jnp.logical_not(on_diagonal))
    def _():
        total = zeros()
        for n in range(blocks):
            times_panel(total, dot(0, 0, width, n), n)
        for r in range(rows):
            parts[r] = total[r] * 2.0

    @pl.when(on_diagonal)
    def _():
        narrow(1)
        gain_own.wait()
        total = zeros()
        for n in range(blocks):
            later = 1 if 2 * n >= blocks else 0
            quarter = jnp.where(side == 0, later, 1 - later) * (width // 2)
            product = dot(0, quarter, width // 2, n)
            if n:
                product += dot(1, 0, n * block_width, n)
            product = product * 2.0 + dot(1, n * block_width, block_width, n)
            times_panel(total, product, n)
        for r in range(rows):
            parts[r] = total[r]

    lane = lax.broadcasted_iota(jnp.int32, (devices, LANES), 1)
    packed = jnp.zeros((devices, LANES), jnp.float32)
    for r in range(rows):
        packed = jnp.where(lane == r, jnp.sum(parts[r], axis=1, keepdims=True), packed)
    for t in range(devices):
        outgoing[t] = packed[t : t + 1]

    def last(dd, db):
        d, b = depth ^ dd, blk ^ db
        return remote(
            outgoing.at[d * blk_count + b], arrived.at[dd * blk_count + db],
            last_send.at[0], last_recv.at[0], d, b,
        )

    for db in reversed(range(blk_count)):
        for dd in reversed(range(depth_count)):
            if dd or db:
                last(dd, db).start()

    own = outgoing[depth * blk_count + blk]

    for sem_at, cond in enumerate((two_up, two_down, plane < end, plane > 0)):
        @pl.when(cond)
        def _():
            settle(lines.at[0], line_send.at[sem_at])

    def relayed(source):
        down, up = relays(source)

        @pl.when(down | up)
        def _():
            settle(lines.at[0], line_send.at[4 + source])

    stages(relayed)
    settle(other_in.at[:, pl.ds(1, group - 1)], other_send.at[0])
    settle(panel_in.at[:, 0, pl.ds(1, half_group - 1)], panel_send.at[0])
    settle(panel_in.at[:, 1], twin_send.at[0])
    settle(arrived.at[pl.ds(1, devices - 1)], last_send.at[0])
    settle(arrived.at[pl.ds(1, devices - 1)], last_recv.at[0])

    total = own
    for t in range(1, devices):
        total += arrived[t]
    out_ref[...] = total


def half_shards(jacobian, gain_inverse, variance):
    rows, states = jacobian.shape
    depth_count = lax.axis_size("depth")
    blk_count = lax.axis_size("blk")
    devices = depth_count * blk_count
    per = blk_count // depth_count
    planes, group = depth_count, depth_count * per
    chunks = states // LANES
    sub = states // blk_count // LANES
    width = sub * LANES
    bf16, f32 = jnp.bfloat16, jnp.float32
    dma = pltpu.SemaphoreType.DMA
    quadratic = pl.pallas_call(
        functools.partial(half_kernel, depth_count, blk_count, rows),
        out_shape=jax.ShapeDtypeStruct((1, LANES), f32),
        in_specs=[pl.BlockSpec(memory_space=pl.ANY)] * 2,
        out_specs=pl.BlockSpec(memory_space=pltpu.VMEM),
        scratch_shapes=[
            pltpu.VMEM((rows, states), bf16),
            pltpu.VMEM((rows * chunks, LANES), f32),
            pltpu.VMEM((planes, rows, chunks, LANES), bf16),
            pltpu.VMEM((planes, group, rows, sub, LANES), bf16),
            pltpu.VMEM((planes, 2, group // 2, rows, sub, LANES), bf16),
            pltpu.VMEM((2, devices * (rows * sub + 1), LANES), f32),
            pltpu.VMEM((2, width, width), bf16),
            pltpu.VMEM((2, rows * devices, width), bf16),
            pltpu.VMEM((rows, devices, LANES), f32),
            pltpu.VMEM((devices, 1, LANES), f32),
            pltpu.VMEM((devices, 1, LANES), f32),
            dma((3,)),
            dma((4 + planes,)),
            dma((planes, planes)),
            dma((1,)),
            dma((planes,)),
            dma((1,)),
            dma((planes,)),
            dma((1,)),
            dma((planes,)),
            dma((1,)),
            dma((1,)),
            pltpu.SemaphoreType.REGULAR((2,)),
        ],
        compiler_params=pltpu.CompilerParams(
            collective_id=0, has_side_effects=True, vmem_limit_bytes=60 * 1024 * 1024
        ),
    )(jacobian, gain_inverse)
    return variance - quadratic[0, :rows]


def solution(mesh):
    in_specs = (P(("depth", "blk"), None), P("depth", "blk"), P(("depth", "blk")))
    out_specs = P(("depth", "blk"))
    depth_count, blk_count = mesh.shape["depth"], mesh.shape["blk"]

    def shards(jacobian, gain_inverse, variance):
        width = gain_inverse.shape[1]
        fits = gain_inverse.size * gain_inverse.dtype.itemsize <= 16 * 1024 * 1024
        paired = depth_count in (2, 4) and blk_count == 2 * depth_count
        if paired and width % (PACKED * LANES) == 0 and fits:
            return half_shards(jacobian, gain_inverse, variance)
        return plain_shards(jacobian, gain_inverse, variance)

    return jax.shard_map(shards, mesh=mesh, in_specs=in_specs, out_specs=out_specs, check_vma=False)
```

```python
import functools

import jax
import jax.numpy as jnp
from jax import lax
from jax.experimental import pallas as pl
from jax.experimental.pallas import tpu as pltpu
from jax.sharding import PartitionSpec as P

LANES = 128
SUBLANES = 8
PACKED = 16
MESH = pl.DeviceIdType.MESH


def exchange_kernel(depth_count, blk_count, slots, *refs):
    count = len(slots)
    sources, targets = refs[:count], refs[count : 2 * count]
    send_sem, recv_sem, own_sem = refs[2 * count :]
    devices = depth_count * blk_count
    me = lax.axis_index("depth") * blk_count + lax.axis_index("blk")

    def place(device):
        return {"depth": device // blk_count, "blk": lax.rem(device, blk_count)}

    def peer(step):
        return lax.rem(me + step, devices)

    def slot_of(kind, device):
        if kind == "depth":
            return device // blk_count
        if kind == "blk":
            return lax.rem(device, blk_count)
        return device

    def copy(which, step):
        device = peer(step)
        return pltpu.make_async_remote_copy(
            src_ref=sources[which].at[slot_of(slots[which], device)],
            dst_ref=targets[which].at[me],
            send_sem=send_sem.at[which, step],
            recv_sem=recv_sem.at[which, step],
            device_id=place(device),
            device_id_type=MESH,
        )

    barrier = pltpu.get_barrier_semaphore()

    @pl.loop(1, devices)
    def _(step):
        pl.semaphore_signal(barrier, inc=1, device_id=place(peer(step)), device_id_type=MESH)

    own = [
        pltpu.make_async_copy(sources[w].at[slot_of(slots[w], me)], targets[w].at[me], own_sem.at[w])
        for w in range(count)
    ]
    for w in range(count):
        own[w].start()
    pl.semaphore_wait(barrier, devices - 1)

    @pl.loop(1, devices)
    def _(step):
        for w in range(count):
            copy(w, step).start()

    for w in range(count):
        own[w].wait()

    @pl.loop(1, devices)
    def _(step):
        for w in range(count):
            copy(w, step).wait()


def exchange(slots, collective_id, *operands):
    depth_count = lax.axis_size("depth")
    blk_count = lax.axis_size("blk")
    devices = depth_count * blk_count
    count = len(slots)
    vmem = pl.BlockSpec(memory_space=pltpu.VMEM)
    return pl.pallas_call(
        functools.partial(exchange_kernel, depth_count, blk_count, slots),
        out_shape=[jax.ShapeDtypeStruct((devices,) + x.shape[1:], x.dtype) for x in operands],
        in_specs=[vmem] * count,
        out_specs=[vmem] * count,
        scratch_shapes=[
            pltpu.SemaphoreType.DMA((count, devices)),
            pltpu.SemaphoreType.DMA((count, devices)),
            pltpu.SemaphoreType.DMA((count,)),
        ],
        compiler_params=pltpu.CompilerParams(collective_id=collective_id, has_side_effects=True),
    )(*operands)


def sections(jacobian, parts):
    rows, states = jacobian.shape
    width = states // parts
    return jacobian.reshape(rows, parts, width // LANES, LANES).transpose(1, 0, 2, 3)


def plain_shards(jacobian, gain_inverse, variance):
    rows = jacobian.shape[0]
    depth_count = lax.axis_size("depth")
    blk_count = lax.axis_size("blk")
    devices = depth_count * blk_count
    left, right = exchange(
        ("depth", "blk"), 0, sections(jacobian, depth_count), sections(jacobian, blk_count)
    )
    left = left.reshape(devices * rows, -1)
    panel = right.reshape(devices * rows, -1)
    projected = jnp.dot(left, gain_inverse, preferred_element_type=jnp.float32)
    partial_sum = jnp.sum(projected * panel.astype(jnp.float32), axis=1)
    padded = jnp.pad(
        partial_sum.reshape(devices, 1, rows), ((0, 0), (0, SUBLANES - 1), (0, LANES - rows))
    )
    (gathered,) = exchange(("all",), 1, padded)
    quadratic = jnp.sum(gathered[:, 0, :rows], axis=0)
    return variance - quadratic


def half_kernel(
    depth_count, blk_count, rows, jac_ref, gain_ref, out_ref,
    own_raw, own_wide, lines, other_in, panel_in, wide, gain, left, projected, outgoing, arrived,
    local_sem, line_send, line_recv, other_send, other_recv,
    panel_send, panel_recv, twin_send, twin_recv, last_send, last_recv,
):
    per = blk_count // depth_count
    planes = depth_count
    group = depth_count * per
    half_group = group // 2
    devices = depth_count * blk_count
    states = jac_ref.shape[1]
    chunks = states // LANES
    sub = states // blk_count // LANES
    width = sub * LANES
    pitch = rows * sub + 1
    end = planes - 1
    depth = lax.axis_index("depth")
    blk = lax.axis_index("blk")
    plane = blk // per
    side = lax.rem(blk, per)
    spot = depth * per + side
    parity = lax.rem(depth, 2)
    twin = depth + 1 - 2 * parity
    seat = (depth // 2) * per + side
    on_diagonal = plane == depth

    def inside(z):
        return (z > 0) & (z < end)

    two_up = inside(plane + 2)
    two_down = inside(plane - 2)

    def wrap(value, count):
        return jnp.where(value >= count, value - count, value)

    def other_section(d, z, s):
        return d * per + jnp.where(d < z, s, per - 1 - s)

    my_other = other_section(depth, plane, side)

    def section_of(source, section):
        return lines.at[source, :, pl.ds(pl.multiple_of(section * sub, sub), sub), :]

    def remote(src, dst, send_sem, recv_sem, d, b):
        return pltpu.make_async_remote_copy(
            src_ref=src, dst_ref=dst, send_sem=send_sem, recv_sem=recv_sem,
            device_id={"depth": d, "blk": b}, device_id_type=MESH,
        )

    def settle(ref, sem):
        pltpu.make_async_copy(ref, ref, sem).wait()

    jac_copy = pltpu.make_async_copy(jac_ref, own_raw, local_sem.at[0])
    jac_copy.start()
    gain_other = pltpu.make_async_copy(
        gain_ref.at[pl.ds(pl.multiple_of((my_other - depth * per) * width, width), width), :],
        gain.at[0], local_sem.at[1],
    )
    gain_own = pltpu.make_async_copy(
        gain_ref.at[pl.ds(pl.multiple_of(side * width, width), width), :], gain.at[1], local_sem.at[2]
    )
    gain_other.start()

    @pl.when(on_diagonal)
    def _():
        gain_own.start()

    barrier = pltpu.get_barrier_semaphore()

    def greet(d, b):
        pl.semaphore_signal(barrier, inc=1, device_id={"depth": d, "blk": b}, device_id_type=MESH)

    for s in range(1, group):
        member = wrap(spot + s, group)
        greet(member // per, plane * per + lax.rem(member, per))

    for away in (1, -1, 2, -2):
        known = (plane + away >= 0) & (plane + away <= end)
        if abs(away) == 2:
            known = known & inside(plane)

        @pl.when(known)
        def _():
            greet(depth, blk + away * per)

    jac_copy.wait()
    for c in range(chunks):
        own_wide[pl.ds(c, rows, stride=chunks), :] = own_raw[:, c * LANES : (c + 1) * LANES].astype(
            jnp.float32
        )
    for r in range(rows):
        lines[plane, r] = own_wide[r * chunks : (r + 1) * chunks, :].astype(jnp.bfloat16)

    heard = group - 1
    for known in (plane > 0, plane < end, two_up, two_down):
        heard = heard + jnp.where(known, 1, 0)
    pl.semaphore_wait(barrier, heard)

    def along(source, part, target, send_sem):
        piece = lines.at[source, :, pl.ds(pl.multiple_of(part * (per * sub), per * sub), per * sub), :]
        return remote(piece, piece, send_sem, line_recv.at[source, part], depth, target * per + side)

    def first_part(source, target):
        relayed = jnp.where(
            (target == 0) & (source > 1), 1, jnp.where((target == end) & (source < end - 1), end - 1, target)
        )
        return wrap(relayed, planes)

    def send_line(target, sem_at):
        @pl.loop(0, planes)
        def _(k):
            part = wrap(first_part(plane, target) + k, planes)
            along(plane, part, target, line_send.at[sem_at]).start()

    def to_other(source, d, s):
        receiver = d * per + s
        seen = spot - receiver
        seen = jnp.where(seen < 0, seen + group, seen)
        return remote(
            section_of(source, other_section(d, plane, s)), other_in.at[source, seen],
            other_send.at[0], other_recv.at[source], d, plane * per + s,
        )

    def to_panel(source, step):
        target = wrap(seat + step, half_group)
        s = lax.rem(target, per)
        return remote(
            section_of(source, plane * per + s), panel_in.at[source, 0, half_group - step],
            panel_send.at[0], panel_recv.at[source], (target // per) * 2 + parity, plane * per + s,
        )

    def own_to_twin(source):
        return remote(
            section_of(source, blk), panel_in.at[source, 1, 0],
            twin_send.at[0], twin_recv.at[source], twin, blk,
        )

    def pass_to_twin(source):
        return remote(
            panel_in.at[source, 0, pl.ds(1, half_group - 1)], panel_in.at[source, 1, pl.ds(1, half_group - 1)],
            twin_send.at[0], twin_recv.at[source], twin, blk,
        )

    def spread(source, part):
        @pl.when(part == plane)
        def _():
            for step in range(1, half_group):
                to_panel(source, step).start()
            own_to_twin(source).start()

        for s in range(per):
            @pl.when((part != depth) | (side != s))
            def _():
                to_other(source, part, s).start()

    def forward_panel(source):
        settle(panel_in.at[source, 0, pl.ds(1, half_group - 1)], panel_recv.at[source])
        pass_to_twin(source).start()

    for sem_at, known, away in ((1, two_down, -2), (3, plane > 0, -1), (2, plane < end, 1), (0, two_up, 2)):
        @pl.when(known)
        def _():
            send_line(plane + away, sem_at)

    @pl.loop(0, planes)
    def _(k):
        spread(plane, wrap(plane + k, planes))

    def relays(source):
        down = (plane == 1) & (source > 1)
        up = (plane == end - 1) & (source < end - 1)
        return down, up

    def stages(act):
        for way in (-1, 1):
            for distance in range(1, planes):
                source = plane + way * distance

                @pl.when((source >= 0) & (source <= end))
                def _():
                    act(source)

    def receive(source):
        down, up = relays(source)

        @pl.loop(0, planes)
        def _(k):
            part = wrap(first_part(source, plane) + k, planes)
            along(source, part, plane, line_send.at[0]).wait_recv()

            @pl.when(down | up)
            def _():
                along(source, part, jnp.where(down, 0, end), line_send.at[4 + source]).start()

            spread(source, part)

    stages(receive)

    def widen(index, slot, block):
        wide[index, pl.ds(slot * pitch, rows * sub), :] = block.reshape(rows * sub, LANES).astype(
            jnp.float32
        )

    def slot_of(source, d, s):
        return d * blk_count + source * per + s

    def collect_other(source):
        widen(0, slot_of(source, depth, side), section_of(source, my_other)[...])
        settle(other_in.at[source, pl.ds(1, group - 1)], other_recv.at[source])

        @pl.loop(1, group)
        def _(k):
            member = wrap(spot + k, group)
            widen(0, slot_of(source, member // per, lax.rem(member, per)), other_in[source, k])

    def collect_panel(source):
        widen(1, slot_of(source, depth, side), section_of(source, blk)[...])
        settle(panel_in.at[source, 1], twin_recv.at[source])

        @pl.loop(0, half_group)
        def _(k):
            at = wrap(seat + k, half_group)
            widen(1, slot_of(source, (at // per) * 2 + 1 - parity, lax.rem(at, per)), panel_in[source, 1, k])

            @pl.when(k > 0)
            def _():
                widen(1, slot_of(source, (at // per) * 2 + parity, lax.rem(at, per)), panel_in[source, 0, k])

    collect_other(plane)
    stages(collect_other)
    forward_panel(plane)
    stages(forward_panel)

    def columns(index, c):
        return [wide[index, pl.ds(r * sub + c, devices, stride=pitch), :] for r in range(rows)]

    def narrow(index):
        for c in range(sub):
            for r, block in enumerate(columns(index, c)):
                left[index, r * devices : (r + 1) * devices, c * LANES : (c + 1) * LANES] = block.astype(
                    jnp.bfloat16
                )

    narrow(0)
    block_width = width // 4
    blocks = width // block_width
    inner = block_width // LANES

    def dot(index, first, count, n):
        if isinstance(first, int):
            a = left[index, :, first : first + count]
        else:
            a = left[index, :, pl.ds(pl.multiple_of(first, LANES), count)]
        b = gain[index, pl.ds(first, count), n * block_width : (n + 1) * block_width]
        return jnp.dot(a, b, preferred_element_type=jnp.float32)

    gain_other.wait()

    @pl.when(jnp.logical_not(on_diagonal))
    def _():
        for n in range(blocks):
            projected[:, n * block_width : (n + 1) * block_width] = dot(0, 0, width, n)

    @pl.when(on_diagonal)
    def _():
        for n in range(blocks):
            later = 1 if 2 * n >= blocks else 0
            quarter = jnp.where(side == 0, later, 1 - later) * (width // 2)
            projected[:, n * block_width : (n + 1) * block_width] = dot(0, quarter, width // 2, n)

    collect_panel(plane)
    stages(collect_panel)

    @pl.when(on_diagonal)
    def _():
        narrow(1)
        gain_own.wait()
        for n in range(blocks):
            at = slice(n * block_width, (n + 1) * block_width)
            if n:
                projected[:, at] += dot(1, 0, n * block_width, n)
            projected[:, at] += dot(1, n * block_width, block_width, n) * 0.5

    total = [jnp.zeros((devices, LANES), jnp.float32) for _ in range(rows)]
    for c in range(sub):
        for r, panel in enumerate(columns(1, c)):
            total[r] += projected[r * devices : (r + 1) * devices, c * LANES : (c + 1) * LANES] * panel

    lane = lax.broadcasted_iota(jnp.int32, (devices, LANES), 1)
    packed = jnp.zeros((devices, LANES), jnp.float32)
    for r in range(rows):
        packed = jnp.where(lane == r, 2.0 * jnp.sum(total[r], axis=1, keepdims=True), packed)
    for t in range(devices):
        outgoing[t] = packed[t : t + 1]

    def last(dd, db):
        d, b = depth ^ dd, blk ^ db
        return remote(
            outgoing.at[d * blk_count + b], arrived.at[dd * blk_count + db],
            last_send.at[0], last_recv.at[0], d, b,
        )

    for db in reversed(range(blk_count)):
        for dd in reversed(range(depth_count)):
            if dd or db:
                last(dd, db).start()

    own = outgoing[depth * blk_count + blk]

    for sem_at, cond in enumerate((two_up, two_down, plane < end, plane > 0)):
        @pl.when(cond)
        def _():
            settle(lines.at[0], line_send.at[sem_at])

    def relayed(source):
        down, up = relays(source)

        @pl.when(down | up)
        def _():
            settle(lines.at[0], line_send.at[4 + source])

    stages(relayed)
    settle(other_in.at[:, pl.ds(1, group - 1)], other_send.at[0])
    settle(panel_in.at[:, 0, pl.ds(1, half_group - 1)], panel_send.at[0])
    settle(panel_in.at[:, 1], twin_send.at[0])
    settle(arrived.at[pl.ds(1, devices - 1)], last_send.at[0])
    settle(arrived.at[pl.ds(1, devices - 1)], last_recv.at[0])

    whole = own
    for t in range(1, devices):
        whole += arrived[t]
    out_ref[...] = whole


def half_shards(jacobian, gain_inverse, variance):
    rows, states = jacobian.shape
    depth_count = lax.axis_size("depth")
    blk_count = lax.axis_size("blk")
    devices = depth_count * blk_count
    per = blk_count // depth_count
    planes, group = depth_count, depth_count * per
    chunks = states // LANES
    sub = states // blk_count // LANES
    width = sub * LANES
    bf16, f32 = jnp.bfloat16, jnp.float32
    dma = pltpu.SemaphoreType.DMA
    quadratic = pl.pallas_call(
        functools.partial(half_kernel, depth_count, blk_count, rows),
        out_shape=jax.ShapeDtypeStruct((1, LANES), f32),
        in_specs=[pl.BlockSpec(memory_space=pl.ANY)] * 2,
        out_specs=pl.BlockSpec(memory_space=pltpu.VMEM),
        scratch_shapes=[
            pltpu.VMEM((rows, states), bf16),
            pltpu.VMEM((rows * chunks, LANES), f32),
            pltpu.VMEM((planes, rows, chunks, LANES), bf16),
            pltpu.VMEM((planes, group, rows, sub, LANES), bf16),
            pltpu.VMEM((planes, 2, group // 2, rows, sub, LANES), bf16),
            pltpu.VMEM((2, devices * (rows * sub + 1), LANES), f32),
            pltpu.VMEM((2, width, width), bf16),
            pltpu.VMEM((2, rows * devices, width), bf16),
            pltpu.VMEM((rows * devices, width), f32),
            pltpu.VMEM((devices, 1, LANES), f32),
            pltpu.VMEM((devices, 1, LANES), f32),
            dma((3,)),
            dma((4 + planes,)),
            dma((planes, planes)),
            dma((1,)),
            dma((planes,)),
            dma((1,)),
            dma((planes,)),
            dma((1,)),
            dma((planes,)),
            dma((1,)),
            dma((1,)),
        ],
        compiler_params=pltpu.CompilerParams(
            collective_id=0, has_side_effects=True, vmem_limit_bytes=60 * 1024 * 1024
        ),
    )(jacobian, gain_inverse)
    return variance - quadratic[0, :rows]


def solution(mesh):
    in_specs = (P(("depth", "blk"), None), P("depth", "blk"), P(("depth", "blk")))
    out_specs = P(("depth", "blk"))
    depth_count, blk_count = mesh.shape["depth"], mesh.shape["blk"]

    def shards(jacobian, gain_inverse, variance):
        width = gain_inverse.shape[1]
        fits = gain_inverse.size * gain_inverse.dtype.itemsize <= 16 * 1024 * 1024
        paired = depth_count in (2, 4) and blk_count == 2 * depth_count
        if paired and width % (PACKED * LANES) == 0 and fits:
            return half_shards(jacobian, gain_inverse, variance)
        return plain_shards(jacobian, gain_inverse, variance)

    return jax.shard_map(shards, mesh=mesh, in_specs=in_specs, out_specs=out_specs, check_vma=False)
```

```python
import functools

import jax
import jax.numpy as jnp
from jax import lax
from jax.experimental import pallas as pl
from jax.experimental.pallas import tpu as pltpu
from jax.sharding import PartitionSpec as P

LANES = 128
SUBLANES = 8
PACKED = 16
MESH = pl.DeviceIdType.MESH


def exchange_kernel(depth_count, blk_count, slots, *refs):
    count = len(slots)
    sources, targets = refs[:count], refs[count : 2 * count]
    send_sem, recv_sem, own_sem = refs[2 * count :]
    devices = depth_count * blk_count
    me = lax.axis_index("depth") * blk_count + lax.axis_index("blk")

    def place(device):
        return {"depth": device // blk_count, "blk": lax.rem(device, blk_count)}

    def peer(step):
        return lax.rem(me + step, devices)

    def slot_of(kind, device):
        if kind == "depth":
            return device // blk_count
        if kind == "blk":
            return lax.rem(device, blk_count)
        return device

    def copy(which, step):
        device = peer(step)
        return pltpu.make_async_remote_copy(
            src_ref=sources[which].at[slot_of(slots[which], device)],
            dst_ref=targets[which].at[me],
            send_sem=send_sem.at[which, step],
            recv_sem=recv_sem.at[which, step],
            device_id=place(device),
            device_id_type=MESH,
        )

    barrier = pltpu.get_barrier_semaphore()

    @pl.loop(1, devices)
    def _(step):
        pl.semaphore_signal(barrier, inc=1, device_id=place(peer(step)), device_id_type=MESH)

    own = [
        pltpu.make_async_copy(sources[w].at[slot_of(slots[w], me)], targets[w].at[me], own_sem.at[w])
        for w in range(count)
    ]
    for w in range(count):
        own[w].start()
    pl.semaphore_wait(barrier, devices - 1)

    @pl.loop(1, devices)
    def _(step):
        for w in range(count):
            copy(w, step).start()

    for w in range(count):
        own[w].wait()

    @pl.loop(1, devices)
    def _(step):
        for w in range(count):
            copy(w, step).wait()


def exchange(slots, collective_id, *operands):
    depth_count = lax.axis_size("depth")
    blk_count = lax.axis_size("blk")
    devices = depth_count * blk_count
    count = len(slots)
    vmem = pl.BlockSpec(memory_space=pltpu.VMEM)
    return pl.pallas_call(
        functools.partial(exchange_kernel, depth_count, blk_count, slots),
        out_shape=[jax.ShapeDtypeStruct((devices,) + x.shape[1:], x.dtype) for x in operands],
        in_specs=[vmem] * count,
        out_specs=[vmem] * count,
        scratch_shapes=[
            pltpu.SemaphoreType.DMA((count, devices)),
            pltpu.SemaphoreType.DMA((count, devices)),
            pltpu.SemaphoreType.DMA((count,)),
        ],
        compiler_params=pltpu.CompilerParams(collective_id=collective_id, has_side_effects=True),
    )(*operands)


def sections(jacobian, parts):
    rows, states = jacobian.shape
    width = states // parts
    return jacobian.reshape(rows, parts, width // LANES, LANES).transpose(1, 0, 2, 3)


def plain_shards(jacobian, gain_inverse, variance):
    rows = jacobian.shape[0]
    depth_count = lax.axis_size("depth")
    blk_count = lax.axis_size("blk")
    devices = depth_count * blk_count
    left, right = exchange(
        ("depth", "blk"), 0, sections(jacobian, depth_count), sections(jacobian, blk_count)
    )
    left = left.reshape(devices * rows, -1)
    panel = right.reshape(devices * rows, -1)
    projected = jnp.dot(left, gain_inverse, preferred_element_type=jnp.float32)
    partial_sum = jnp.sum(projected * panel.astype(jnp.float32), axis=1)
    padded = jnp.pad(
        partial_sum.reshape(devices, 1, rows), ((0, 0), (0, SUBLANES - 1), (0, LANES - rows))
    )
    (gathered,) = exchange(("all",), 1, padded)
    quadratic = jnp.sum(gathered[:, 0, :rows], axis=0)
    return variance - quadratic


def half_kernel(
    depth_count, blk_count, rows, jac_ref, gain_ref, out_ref,
    own_raw, own_wide, lines, other_in, panel_in, wide, gain, left, projected, partial, outgoing, arrived,
    local_sem, line_send, line_recv, other_send, other_recv,
    panel_send, panel_recv, twin_send, twin_recv, last_send, last_recv,
):
    per = blk_count // depth_count
    planes = depth_count
    group = depth_count * per
    half_group = group // 2
    devices = depth_count * blk_count
    states = jac_ref.shape[1]
    chunks = states // LANES
    sub = states // blk_count // LANES
    width = sub * LANES
    pitch = rows * sub + 1
    end = planes - 1
    depth = lax.axis_index("depth")
    blk = lax.axis_index("blk")
    plane = blk // per
    side = lax.rem(blk, per)
    spot = depth * per + side
    parity = lax.rem(depth, 2)
    twin = depth + 1 - 2 * parity
    seat = (depth // 2) * per + side
    on_diagonal = plane == depth

    def at_end(z):
        return (z == 0) | (z == end)

    def adjacent(d, z):
        return (d - z == 1) | (z - d == 1)

    def takes_none(d, z):
        return adjacent(d, z) & at_end(z)

    def takes_both(d, z):
        return adjacent(d, z) & at_end(d)

    idle = takes_none(depth, plane)
    double = takes_both(depth, plane)
    single = jnp.logical_not(idle | double)
    sources = [jnp.where(i < plane, plane - 1 - i, i + 1) for i in range(planes - 1)]

    def inside(z):
        return (z > 0) & (z < end)

    two_up = inside(plane + 2)
    two_down = inside(plane - 2)

    def wrap(value, count):
        return jnp.where(value >= count, value - count, value)

    def other_section(d, z, s):
        return d * per + jnp.where(d < z, s, per - 1 - s)

    my_other = other_section(depth, plane, side)

    def section_of(source, section):
        return lines.at[source, :, pl.ds(pl.multiple_of(section * sub, sub), sub), :]

    def remote(src, dst, send_sem, recv_sem, d, b):
        return pltpu.make_async_remote_copy(
            src_ref=src, dst_ref=dst, send_sem=send_sem, recv_sem=recv_sem,
            device_id={"depth": d, "blk": b}, device_id_type=MESH,
        )

    def settle(ref, sem):
        pltpu.make_async_copy(ref, ref, sem).wait()

    jac_copy = pltpu.make_async_copy(jac_ref, own_raw, local_sem.at[0])
    jac_copy.start()
    gain_first = pltpu.make_async_copy(
        gain_ref.at[pl.ds(pl.multiple_of(jnp.where(double, 0, my_other - depth * per) * width, width), width), :],
        gain.at[0], local_sem.at[1],
    )
    gain_second = pltpu.make_async_copy(
        gain_ref.at[pl.ds(pl.multiple_of(jnp.where(double, 1, side) * width, width), width), :],
        gain.at[1], local_sem.at[2],
    )

    @pl.when(jnp.logical_not(idle))
    def _():
        gain_first.start()

    @pl.when(on_diagonal | double)
    def _():
        gain_second.start()

    barrier = pltpu.get_barrier_semaphore()

    def greet(d, b):
        pl.semaphore_signal(barrier, inc=1, device_id={"depth": d, "blk": b}, device_id_type=MESH)

    for s in range(1, group):
        member = wrap(spot + s, group)
        greet(member // per, plane * per + lax.rem(member, per))

    for away in (1, -1, 2, -2):
        known = (plane + away >= 0) & (plane + away <= end)
        if abs(away) == 2:
            known = known & inside(plane)

        @pl.when(known)
        def _():
            greet(depth, blk + away * per)

    jac_copy.wait()
    for c in range(chunks):
        own_wide[pl.ds(c, rows, stride=chunks), :] = own_raw[:, c * LANES : (c + 1) * LANES].astype(
            jnp.float32
        )
    for r in range(rows):
        lines[plane, r] = own_wide[r * chunks : (r + 1) * chunks, :].astype(jnp.bfloat16)

    heard = group - 1
    for known in (plane > 0, plane < end, two_up, two_down):
        heard = heard + jnp.where(known, 1, 0)
    pl.semaphore_wait(barrier, heard)

    def along(source, part, target, send_sem):
        piece = lines.at[source, :, pl.ds(pl.multiple_of(part * (per * sub), per * sub), per * sub), :]
        return remote(piece, piece, send_sem, line_recv.at[source, part], depth, target * per + side)

    def first_part(target):
        return wrap(jnp.clip(target, 1, end - 1) + 1, planes)

    def part_count(target):
        return jnp.where(at_end(target), planes - 1, planes)

    def send_line(target, sem_at):
        @pl.loop(0, part_count(target))
        def _(k):
            along(plane, wrap(first_part(target) + k, planes), target, line_send.at[sem_at]).start()

    def seen_from(d, s):
        seen = spot - (d * per + s)
        return jnp.where(seen < 0, seen + group, seen)

    def to_other(source, d, s):
        return remote(
            section_of(source, other_section(d, plane, s)),
            other_in.at[source, seen_from(d, s), :, pl.ds(0, sub)],
            other_send.at[d], other_recv.at[source], d, plane * per + s,
        )

    def to_both(source, d, s):
        return remote(
            lines.at[source, :, pl.ds(pl.multiple_of(d * per * sub, per * sub), per * sub), :],
            other_in.at[source, seen_from(d, s)],
            other_send.at[d], other_recv.at[source], d, plane * per + s,
        )

    def to_panel(source, step):
        target = wrap(seat + step, half_group)
        s = lax.rem(target, per)
        return remote(
            section_of(source, plane * per + s), panel_in.at[source, 0, half_group - step],
            panel_send.at[0], panel_recv.at[source], (target // per) * 2 + parity, plane * per + s,
        )

    def own_to_twin(source):
        return remote(
            section_of(source, blk), panel_in.at[source, 1, 0],
            twin_send.at[0], twin_recv.at[source], twin, blk,
        )

    def pass_to_twin(source):
        return remote(
            panel_in.at[source, 0, pl.ds(1, half_group - 1)], panel_in.at[source, 1, pl.ds(1, half_group - 1)],
            twin_send.at[0], twin_recv.at[source], twin, blk,
        )

    def spread(source, part):
        @pl.when(part == plane)
        def _():
            for step in range(1, half_group):
                to_panel(source, step).start()
            own_to_twin(source).start()

        for s in range(per):
            foreign = (part != depth) | (side != s)

            @pl.when(foreign & takes_both(part, plane))
            def _():
                to_both(source, part, s).start()

            @pl.when(foreign & jnp.logical_not(adjacent(part, plane) & (at_end(part) | at_end(plane))))
            def _():
                to_other(source, part, s).start()

    def forward_panel(source):
        settle(panel_in.at[source, 0, pl.ds(1, half_group - 1)], panel_recv.at[source])
        pass_to_twin(source).start()

    for sem_at, known, away in ((1, two_down, -2), (3, plane > 0, -1), (2, plane < end, 1), (0, two_up, 2)):
        @pl.when(known)
        def _():
            send_line(plane + away, sem_at)

    @pl.loop(0, planes)
    def _(k):
        spread(plane, wrap(plane + k, planes))

    def relays(source):
        down = (plane == 1) & (source > 1)
        up = (plane == end - 1) & (source < end - 1)
        return down, up

    def receive(source, k):
        down, up = relays(source)
        part = wrap(first_part(plane) + k, planes)
        along(source, part, plane, line_send.at[0]).wait_recv()

        @pl.when((down | up) & (k < planes - 1))
        def _():
            along(source, part, jnp.where(down, 0, end), line_send.at[4 + source]).start()

        spread(source, part)

    @pl.when(at_end(plane))
    def _():
        for source in sources:
            @pl.loop(0, planes - 1)
            def _(k):
                receive(source, k)

    @pl.when(jnp.logical_not(at_end(plane)))
    def _():
        for turn in (sources[:2], sources[2:]):
            @pl.loop(0, planes)
            def _(k):
                for source in turn:
                    receive(source, k)

    def widen(index, slot, block):
        wide[index, pl.ds(slot * pitch, rows * sub), :] = block.reshape(rows * sub, LANES).astype(
            jnp.float32
        )

    def slot_of(source, d, s):
        return d * blk_count + source * per + s

    def collect_other(source):
        slot = slot_of(source, depth, side)

        def gather(first_section, count, indices):
            settle(other_in.at[source, pl.ds(1, group - 1), :, pl.ds(0, count * sub)], other_recv.at[source])
            for n, index in enumerate(indices):
                widen(index, slot, section_of(source, first_section + n)[...])

            @pl.loop(1, group)
            def _(k):
                member = wrap(spot + k, group)
                at = slot_of(source, member // per, lax.rem(member, per))
                for n, index in enumerate(indices):
                    widen(index, at, other_in[source, k, :, n * sub : (n + 1) * sub])

        @pl.when(single)
        def _():
            gather(my_other, 1, (0,))

        @pl.when(double)
        def _():
            gather(depth * per, 2, (0, 2))

    def collect_panel(source):
        widen(1, slot_of(source, depth, side), section_of(source, blk)[...])
        settle(panel_in.at[source, 1], twin_recv.at[source])

        @pl.loop(0, half_group)
        def _(k):
            at = wrap(seat + k, half_group)
            widen(1, slot_of(source, (at // per) * 2 + 1 - parity, lax.rem(at, per)), panel_in[source, 1, k])

            @pl.when(k > 0)
            def _():
                widen(1, slot_of(source, (at // per) * 2 + parity, lax.rem(at, per)), panel_in[source, 0, k])

    everything = [plane] + sources
    for source in everything:
        collect_other(source)
    for source in everything:
        forward_panel(source)

    def columns(index, c):
        return [wide[index, pl.ds(r * sub + c, devices, stride=pitch), :] for r in range(rows)]

    def narrow(index, source):
        for c in range(sub):
            for r, block in enumerate(columns(source, c)):
                left[index, r * devices : (r + 1) * devices, c * LANES : (c + 1) * LANES] = block.astype(
                    jnp.bfloat16
                )

    block_width = width // 4
    blocks = width // block_width
    inner = block_width // LANES

    def dot(index, first, count, n):
        if isinstance(first, int):
            a = left[index, :, first : first + count]
        else:
            a = left[index, :, pl.ds(pl.multiple_of(first, LANES), count)]
        b = gain[index, pl.ds(first, count), n * block_width : (n + 1) * block_width]
        return jnp.dot(a, b, preferred_element_type=jnp.float32)

    def columns_of(n):
        return slice(n * block_width, (n + 1) * block_width)

    @pl.when(jnp.logical_not(idle))
    def _():
        narrow(0, 0)
        gain_first.wait()

    @pl.when(single & jnp.logical_not(on_diagonal))
    def _():
        for n in range(blocks):
            projected[:, columns_of(n)] = dot(0, 0, width, n)

    @pl.when(double)
    def _():
        narrow(1, 2)
        gain_second.wait()
        for n in range(blocks):
            projected[:, columns_of(n)] = dot(0, 0, width, n) + dot(1, 0, width, n)

    @pl.when(on_diagonal)
    def _():
        for n in range(blocks):
            later = 1 if 2 * n >= blocks else 0
            quarter = jnp.where(side == 0, later, 1 - later) * (width // 2)
            projected[:, columns_of(n)] = dot(0, quarter, width // 2, n)

    for source in everything:
        collect_panel(source)

    @pl.when(on_diagonal)
    def _():
        narrow(1, 1)
        gain_second.wait()
        for n in range(blocks):
            at = columns_of(n)
            if n:
                projected[:, at] += dot(1, 0, n * block_width, n)
            projected[:, at] += dot(1, n * block_width, block_width, n) * 0.5

    @pl.when(idle)
    def _():
        partial[...] = jnp.zeros_like(partial)

    @pl.when(jnp.logical_not(idle))
    def _():
        total = [jnp.zeros((devices, LANES), jnp.float32) for _ in range(rows)]
        for c in range(sub):
            for r, panel in enumerate(columns(1, c)):
                total[r] += projected[r * devices : (r + 1) * devices, c * LANES : (c + 1) * LANES] * panel
        for r in range(rows):
            partial[r] = total[r]

    lane = lax.broadcasted_iota(jnp.int32, (devices, LANES), 1)
    packed = jnp.zeros((devices, LANES), jnp.float32)
    for r in range(rows):
        packed = jnp.where(lane == r, 2.0 * jnp.sum(partial[r], axis=1, keepdims=True), packed)
    for t in range(devices):
        outgoing[t] = packed[t : t + 1]

    def last(dd, db):
        d, b = depth ^ dd, blk ^ db
        return remote(
            outgoing.at[d * blk_count + b], arrived.at[dd * blk_count + db],
            last_send.at[0], last_recv.at[0], d, b,
        )

    for db in reversed(range(blk_count)):
        for dd in reversed(range(depth_count)):
            if dd or db:
                last(dd, db).start()

    own = outgoing[depth * blk_count + blk]

    def line_left(cond, target, sem):
        @pl.when(cond & at_end(target))
        def _():
            settle(lines.at[0, :, pl.ds(0, (planes - 1) * per * sub)], sem)

        @pl.when(cond & jnp.logical_not(at_end(target)))
        def _():
            settle(lines.at[0], sem)

    for sem_at, known, away in ((1, two_down, -2), (3, plane > 0, -1), (2, plane < end, 1), (0, two_up, 2)):
        line_left(known, plane + away, line_send.at[sem_at])

    for source in sources:
        down, up = relays(source)
        line_left(down | up, 0, line_send.at[4 + source])

    for d in range(depth_count):
        for members, here in ((per - 1, depth == d), (per, depth != d)):
            both = takes_both(d, plane)
            for count, taken in ((2, both), (1, jnp.logical_not(both | takes_none(d, plane)))):
                @pl.when(here & taken)
                def _():
                    settle(other_in.at[:, pl.ds(0, members), :, pl.ds(0, count * sub)], other_send.at[d])

    settle(panel_in.at[:, 0, pl.ds(1, half_group - 1)], panel_send.at[0])
    settle(panel_in.at[:, 1], twin_send.at[0])
    settle(arrived.at[pl.ds(1, devices - 1)], last_send.at[0])
    settle(arrived.at[pl.ds(1, devices - 1)], last_recv.at[0])

    whole = own
    for t in range(1, devices):
        whole += arrived[t]
    out_ref[...] = whole


def half_shards(jacobian, gain_inverse, variance):
    rows, states = jacobian.shape
    depth_count = lax.axis_size("depth")
    blk_count = lax.axis_size("blk")
    devices = depth_count * blk_count
    per = blk_count // depth_count
    planes, group = depth_count, depth_count * per
    chunks = states // LANES
    sub = states // blk_count // LANES
    width = sub * LANES
    bf16, f32 = jnp.bfloat16, jnp.float32
    dma = pltpu.SemaphoreType.DMA
    quadratic = pl.pallas_call(
        functools.partial(half_kernel, depth_count, blk_count, rows),
        out_shape=pltpu.VMEM((1, LANES), f32),
        in_specs=[pl.BlockSpec(memory_space=pl.ANY)] * 2,
        out_specs=pl.BlockSpec(memory_space=pltpu.VMEM),
        scratch_shapes=[
            pltpu.VMEM((rows, states), bf16),
            pltpu.VMEM((rows * chunks, LANES), f32),
            pltpu.VMEM((planes, rows, chunks, LANES), bf16),
            pltpu.VMEM((planes, group, rows, per * sub, LANES), bf16),
            pltpu.VMEM((planes, 2, group // 2, rows, sub, LANES), bf16),
            pltpu.VMEM((3, devices * (rows * sub + 1), LANES), f32),
            pltpu.VMEM((2, width, width), bf16),
            pltpu.VMEM((2, rows * devices, width), bf16),
            pltpu.VMEM((rows * devices, width), f32),
            pltpu.VMEM((rows, devices, LANES), f32),
            pltpu.VMEM((devices, 1, LANES), f32),
            pltpu.VMEM((devices, 1, LANES), f32),
            dma((3,)),
            dma((4 + planes,)),
            dma((planes, planes)),
            dma((depth_count,)),
            dma((planes,)),
            dma((1,)),
            dma((planes,)),
            dma((1,)),
            dma((planes,)),
            dma((1,)),
            dma((1,)),
        ],
        compiler_params=pltpu.CompilerParams(
            collective_id=0, has_side_effects=True, vmem_limit_bytes=60 * 1024 * 1024
        ),
    )(jacobian, gain_inverse)
    return variance - quadratic[0, :rows]


def solution(mesh):
    in_specs = (P(("depth", "blk"), None), P("depth", "blk"), P(("depth", "blk")))
    out_specs = P(("depth", "blk"))
    depth_count, blk_count = mesh.shape["depth"], mesh.shape["blk"]

    def shards(jacobian, gain_inverse, variance):
        width = gain_inverse.shape[1]
        fits = gain_inverse.size * gain_inverse.dtype.itemsize <= 16 * 1024 * 1024
        paired = 2 < depth_count <= 4 and depth_count % 2 == 0 and blk_count == 2 * depth_count
        if paired and width % (PACKED * LANES) == 0 and fits:
            return half_shards(jacobian, gain_inverse, variance)
        return plain_shards(jacobian, gain_inverse, variance)

    return jax.shard_map(shards, mesh=mesh, in_specs=in_specs, out_specs=out_specs, check_vma=False)
```

```python
import functools

import jax
import jax.numpy as jnp
from jax import lax
from jax.experimental import pallas as pl
from jax.experimental.pallas import tpu as pltpu
from jax.sharding import PartitionSpec as P

LANES = 128
SUBLANES = 8
PACKED = 16
MESH = pl.DeviceIdType.MESH


def exchange_kernel(depth_count, blk_count, slots, *refs):
    count = len(slots)
    sources, targets = refs[:count], refs[count : 2 * count]
    send_sem, recv_sem, own_sem = refs[2 * count :]
    devices = depth_count * blk_count
    me = lax.axis_index("depth") * blk_count + lax.axis_index("blk")

    def place(device):
        return {"depth": device // blk_count, "blk": lax.rem(device, blk_count)}

    def peer(step):
        return lax.rem(me + step, devices)

    def slot_of(kind, device):
        if kind == "depth":
            return device // blk_count
        if kind == "blk":
            return lax.rem(device, blk_count)
        return device

    def copy(which, step):
        device = peer(step)
        return pltpu.make_async_remote_copy(
            src_ref=sources[which].at[slot_of(slots[which], device)],
            dst_ref=targets[which].at[me],
            send_sem=send_sem.at[which, step],
            recv_sem=recv_sem.at[which, step],
            device_id=place(device),
            device_id_type=MESH,
        )

    barrier = pltpu.get_barrier_semaphore()

    @pl.loop(1, devices)
    def _(step):
        pl.semaphore_signal(barrier, inc=1, device_id=place(peer(step)), device_id_type=MESH)

    own = [
        pltpu.make_async_copy(sources[w].at[slot_of(slots[w], me)], targets[w].at[me], own_sem.at[w])
        for w in range(count)
    ]
    for w in range(count):
        own[w].start()
    pl.semaphore_wait(barrier, devices - 1)

    @pl.loop(1, devices)
    def _(step):
        for w in range(count):
            copy(w, step).start()

    for w in range(count):
        own[w].wait()

    @pl.loop(1, devices)
    def _(step):
        for w in range(count):
            copy(w, step).wait()


def exchange(slots, collective_id, *operands):
    depth_count = lax.axis_size("depth")
    blk_count = lax.axis_size("blk")
    devices = depth_count * blk_count
    count = len(slots)
    vmem = pl.BlockSpec(memory_space=pltpu.VMEM)
    return pl.pallas_call(
        functools.partial(exchange_kernel, depth_count, blk_count, slots),
        out_shape=[jax.ShapeDtypeStruct((devices,) + x.shape[1:], x.dtype) for x in operands],
        in_specs=[vmem] * count,
        out_specs=[vmem] * count,
        scratch_shapes=[
            pltpu.SemaphoreType.DMA((count, devices)),
            pltpu.SemaphoreType.DMA((count, devices)),
            pltpu.SemaphoreType.DMA((count,)),
        ],
        compiler_params=pltpu.CompilerParams(collective_id=collective_id, has_side_effects=True),
    )(*operands)


def sections(jacobian, parts):
    rows, states = jacobian.shape
    width = states // parts
    return jacobian.reshape(rows, parts, width // LANES, LANES).transpose(1, 0, 2, 3)


def plain_shards(jacobian, gain_inverse, variance):
    rows = jacobian.shape[0]
    depth_count = lax.axis_size("depth")
    blk_count = lax.axis_size("blk")
    devices = depth_count * blk_count
    left, right = exchange(
        ("depth", "blk"), 0, sections(jacobian, depth_count), sections(jacobian, blk_count)
    )
    left = left.reshape(devices * rows, -1)
    panel = right.reshape(devices * rows, -1)
    projected = jnp.dot(left, gain_inverse, preferred_element_type=jnp.float32)
    partial_sum = jnp.sum(projected * panel.astype(jnp.float32), axis=1)
    padded = jnp.pad(
        partial_sum.reshape(devices, 1, rows), ((0, 0), (0, SUBLANES - 1), (0, LANES - rows))
    )
    (gathered,) = exchange(("all",), 1, padded)
    quadratic = jnp.sum(gathered[:, 0, :rows], axis=0)
    return variance - quadratic


def half_kernel(
    depth_count, blk_count, rows, jac_ref, gain_ref, out_ref,
    own_raw, own_wide, lines, other_in, panel_in, wide, gain, left, projected, partial, outgoing, arrived,
    local_sem, line_send, line_recv, other_send, other_recv,
    panel_send, panel_recv, twin_send, twin_recv, last_send, last_recv,
):
    per = blk_count // depth_count
    planes = depth_count
    group = depth_count * per
    half_group = group // 2
    devices = depth_count * blk_count
    states = jac_ref.shape[1]
    chunks = states // LANES
    sub = states // blk_count // LANES
    width = sub * LANES
    pitch = rows * sub + 1
    end = planes - 1
    depth = lax.axis_index("depth")
    blk = lax.axis_index("blk")
    plane = blk // per
    side = lax.rem(blk, per)
    spot = depth * per + side
    parity = lax.rem(depth, 2)
    twin = depth + 1 - 2 * parity
    seat = (depth // 2) * per + side
    on_diagonal = plane == depth

    def at_end(z):
        return (z == 0) | (z == end)

    def takes_none(d, z):
        return at_end(z) & jnp.logical_not(at_end(d))

    def takes_both(d, z):
        return at_end(d) & jnp.logical_not(at_end(z))

    idle = takes_none(depth, plane)
    double = takes_both(depth, plane)
    single = jnp.logical_not(idle | double)
    sources = [jnp.where(i < plane, plane - 1 - i, i + 1) for i in range(planes - 1)]

    def inside(z):
        return (z > 0) & (z < end)

    two_up = inside(plane + 2)
    two_down = inside(plane - 2)

    def wrap(value, count):
        return jnp.where(value >= count, value - count, value)

    def other_section(d, z, s):
        return d * per + jnp.where(d < z, s, per - 1 - s)

    my_other = other_section(depth, plane, side)

    def section_of(source, section):
        return lines.at[source, :, pl.ds(pl.multiple_of(section * sub, sub), sub), :]

    def remote(src, dst, send_sem, recv_sem, d, b):
        return pltpu.make_async_remote_copy(
            src_ref=src, dst_ref=dst, send_sem=send_sem, recv_sem=recv_sem,
            device_id={"depth": d, "blk": b}, device_id_type=MESH,
        )

    def settle(ref, sem):
        pltpu.make_async_copy(ref, ref, sem).wait()

    jac_copy = pltpu.make_async_copy(jac_ref, own_raw, local_sem.at[0])
    jac_copy.start()
    gain_first = pltpu.make_async_copy(
        gain_ref.at[pl.ds(pl.multiple_of(jnp.where(double, 0, my_other - depth * per) * width, width), width), :],
        gain.at[pl.ds(0, width)], local_sem.at[1],
    )
    gain_second = pltpu.make_async_copy(
        gain_ref.at[pl.ds(pl.multiple_of(jnp.where(double, 1, side) * width, width), width), :],
        gain.at[pl.ds(width, width)], local_sem.at[2],
    )

    @pl.when(jnp.logical_not(idle))
    def _():
        gain_first.start()

    @pl.when(on_diagonal | double)
    def _():
        gain_second.start()

    barrier = pltpu.get_barrier_semaphore()

    def greet(d, b):
        pl.semaphore_signal(barrier, inc=1, device_id={"depth": d, "blk": b}, device_id_type=MESH)

    for s in range(1, group):
        member = wrap(spot + s, group)
        greet(member // per, plane * per + lax.rem(member, per))

    for away in (1, -1, 2, -2):
        known = (plane + away >= 0) & (plane + away <= end)
        if abs(away) == 2:
            known = known & inside(plane)

        @pl.when(known)
        def _():
            greet(depth, blk + away * per)

    jac_copy.wait()
    for c in range(chunks):
        own_wide[pl.ds(c, rows, stride=chunks), :] = own_raw[:, c * LANES : (c + 1) * LANES].astype(
            jnp.float32
        )
    for r in range(rows):
        lines[plane, r] = own_wide[r * chunks : (r + 1) * chunks, :].astype(jnp.bfloat16)

    heard = group - 1
    for known in (plane > 0, plane < end, two_up, two_down):
        heard = heard + jnp.where(known, 1, 0)
    pl.semaphore_wait(barrier, heard)

    def along(source, part, target, send_sem):
        piece = lines.at[source, :, pl.ds(pl.multiple_of(part * (per * sub), per * sub), per * sub), :]
        return remote(piece, piece, send_sem, line_recv.at[source, part], depth, target * per + side)

    def nth_part(target, k):
        return jnp.where(2 * target < planes, wrap(planes - k, planes), wrap(end + k, planes))

    def part_count(target):
        return jnp.where(at_end(target), 2, planes)

    def send_line(target, sem_at, first, last):
        @pl.loop(first, last)
        def _(k):
            along(plane, nth_part(target, k), target, line_send.at[sem_at]).start()

    def seen_from(d, s):
        seen = spot - (d * per + s)
        return jnp.where(seen < 0, seen + group, seen)

    def to_other(source, d, s):
        return remote(
            section_of(source, other_section(d, plane, s)),
            other_in.at[source, seen_from(d, s), :, pl.ds(0, sub)],
            other_send.at[d], other_recv.at[source], d, plane * per + s,
        )

    def to_both(source, d, s):
        return remote(
            lines.at[source, :, pl.ds(pl.multiple_of(d * per * sub, per * sub), per * sub), :],
            other_in.at[source, seen_from(d, s)],
            other_send.at[d], other_recv.at[source], d, plane * per + s,
        )

    def to_panel(source, step):
        target = wrap(seat + step, half_group)
        s = lax.rem(target, per)
        return remote(
            section_of(source, plane * per + s), panel_in.at[source, 0, half_group - step],
            panel_send.at[0], panel_recv.at[source], (target // per) * 2 + parity, plane * per + s,
        )

    def own_to_twin(source):
        return remote(
            section_of(source, blk), panel_in.at[source, 1, 0],
            twin_send.at[0], twin_recv.at[source], twin, blk,
        )

    def pass_to_twin(source):
        return remote(
            panel_in.at[source, 0, pl.ds(1, half_group - 1)], panel_in.at[source, 1, pl.ds(1, half_group - 1)],
            twin_send.at[0], twin_recv.at[source], twin, blk,
        )

    def spread(source, part):
        for s in range(per):
            foreign = (part != depth) | (side != s)

            @pl.when(foreign & takes_both(part, plane))
            def _():
                to_both(source, part, s).start()

            @pl.when(foreign & (at_end(part) == at_end(plane)))
            def _():
                to_other(source, part, s).start()

    def spread_panel(source):
        for step in range(1, half_group):
            to_panel(source, step).start()
        own_to_twin(source).start()

    def forward_panel(source):
        settle(panel_in.at[source, 0, pl.ds(1, half_group - 1)], panel_recv.at[source])
        pass_to_twin(source).start()

    for sem_at, known, away in ((1, two_down, -2), (3, plane > 0, -1), (2, plane < end, 1), (0, two_up, 2)):
        @pl.when(known)
        def _():
            send_line(plane + away, sem_at, 0, 2)

    @pl.loop(0, planes)
    def _(k):
        spread(plane, nth_part(plane, k))

    spread_panel(plane)

    def relays(source):
        down = (plane == 1) & (source > 1)
        up = (plane == end - 1) & (source < end - 1)
        return down, up

    def send_rest():
        for sem_at, known, away in ((1, two_down, -2), (3, plane > 0, -1), (2, plane < end, 1), (0, two_up, 2)):
            @pl.when(known & jnp.logical_not(at_end(plane + away)))
            def _():
                send_line(plane + away, sem_at, 2, planes)

    def receive(source, k):
        down, up = relays(source)
        part = nth_part(plane, k)
        along(source, part, plane, line_send.at[0]).wait_recv()

        @pl.when((down | up) & (k < 2))
        def _():
            along(source, part, jnp.where(down, 0, end), line_send.at[4 + source]).start()

        spread(source, part)

    @pl.when(at_end(plane))
    def _():
        for n, source in enumerate(sources):
            @pl.loop(0, 2)
            def _(k):
                receive(source, k)
                if n == 0:
                    @pl.when(k == 0)
                    def _():
                        send_rest()

            if n:
                spread_panel(sources[n - 1])

        spread_panel(sources[-1])

    @pl.when(jnp.logical_not(at_end(plane)))
    def _():
        receive(sources[0], 0)
        send_rest()
        receive(sources[1], 0)
        for first, last in ((1, 2), (2, planes)):
            for turn, start in ((sources[:2], first), (sources[2:], first - first % 2)):
                @pl.loop(start, last)
                def _(k):
                    for source in turn:
                        receive(source, k)

        for source in sources:
            spread_panel(source)

    def widen(index, slot, block):
        wide[index, pl.ds(slot * pitch, rows * sub), :] = block.reshape(rows * sub, LANES).astype(
            jnp.float32
        )

    def slot_of(source, d, s):
        return d * blk_count + source * per + s

    def collect_other(source):
        slot = slot_of(source, depth, side)

        def gather(first_section, count, indices):
            settle(other_in.at[source, pl.ds(1, group - 1), :, pl.ds(0, count * sub)], other_recv.at[source])
            for n, index in enumerate(indices):
                widen(index, slot, section_of(source, first_section + n)[...])

            @pl.loop(1, group)
            def _(k):
                member = wrap(spot + k, group)
                at = slot_of(source, member // per, lax.rem(member, per))
                for n, index in enumerate(indices):
                    widen(index, at, other_in[source, k, :, n * sub : (n + 1) * sub])

        @pl.when(single)
        def _():
            gather(my_other, 1, (0,))

        @pl.when(double)
        def _():
            gather(depth * per, 2, (0, 2))

    def collect_panel(source):
        widen(1, slot_of(source, depth, side), section_of(source, blk)[...])
        settle(panel_in.at[source, 1], twin_recv.at[source])

        @pl.loop(0, half_group)
        def _(k):
            at = wrap(seat + k, half_group)
            widen(1, slot_of(source, (at // per) * 2 + 1 - parity, lax.rem(at, per)), panel_in[source, 1, k])

            @pl.when(k > 0)
            def _():
                widen(1, slot_of(source, (at // per) * 2 + parity, lax.rem(at, per)), panel_in[source, 0, k])

    everything = [plane] + sources
    for source in everything:
        collect_other(source)

    def columns(index, c):
        return [wide[index, pl.ds(r * sub + c, devices, stride=pitch), :] for r in range(rows)]

    def narrow(first, source):
        for c in range(sub):
            for r, block in enumerate(columns(source, c)):
                left[r * devices : (r + 1) * devices, first + c * LANES : first + (c + 1) * LANES] = block.astype(
                    jnp.bfloat16
                )

    def dot(first, count, n=slice(0, width)):
        a = left[:, pl.ds(first, count)]
        return jnp.dot(a, gain[pl.ds(first, count), n], preferred_element_type=jnp.float32)

    half = width // 2
    halves = [slice(0, half), slice(half, width)]

    @pl.when(jnp.logical_not(idle))
    def _():
        narrow(0, 0)
        gain_first.wait()

    @pl.when(double)
    def _():
        narrow(width, 2)
        gain_second.wait()

    def multiply(n):
        at = halves[n]

        @pl.when(single & jnp.logical_not(on_diagonal))
        def _():
            projected[:, at] = dot(0, width, at)

        @pl.when(double)
        def _():
            projected[:, at] = dot(0, 2 * width, at)

        @pl.when(on_diagonal)
        def _():
            quarter = pl.multiple_of(jnp.where(side == 0, n, 1 - n) * half, half)
            projected[:, at] = dot(quarter, half, at)

    multiply(0)
    for source in everything:
        forward_panel(source)
    multiply(1)
    for source in everything:
        collect_panel(source)

    @pl.when(on_diagonal)
    def _():
        narrow(width, 1)
        gain_second.wait()
        projected[:, halves[0]] += 0.5 * dot(width, half, halves[0])
        projected[:, halves[1]] += dot(width, half, halves[1]) + 0.5 * dot(width + half, half, halves[1])

    @pl.when(idle)
    def _():
        partial[...] = jnp.zeros_like(partial)

    @pl.when(jnp.logical_not(idle))
    def _():
        total = [jnp.zeros((devices, LANES), jnp.float32) for _ in range(rows)]
        for c in range(sub):
            for r, panel in enumerate(columns(1, c)):
                total[r] += projected[r * devices : (r + 1) * devices, c * LANES : (c + 1) * LANES] * panel
        for r in range(rows):
            partial[r] = total[r]

    lane = lax.broadcasted_iota(jnp.int32, (devices, LANES), 1)
    packed = jnp.zeros((devices, LANES), jnp.float32)
    for r in range(rows):
        packed = jnp.where(lane == r, 2.0 * jnp.sum(partial[r], axis=1, keepdims=True), packed)
    for t in range(devices):
        outgoing[t] = packed[t : t + 1]

    def last(dd, db):
        d, b = depth ^ dd, blk ^ db
        return remote(
            outgoing.at[d * blk_count + b], arrived.at[dd * blk_count + db],
            last_send.at[0], last_recv.at[0], d, b,
        )

    for db in reversed(range(blk_count)):
        for dd in reversed(range(depth_count)):
            if dd or db:
                last(dd, db).start()

    own = outgoing[depth * blk_count + blk]

    def line_left(cond, target, sem):
        @pl.when(cond & at_end(target))
        def _():
            settle(lines.at[0, :, pl.ds(0, 2 * per * sub)], sem)

        @pl.when(cond & jnp.logical_not(at_end(target)))
        def _():
            settle(lines.at[0], sem)

    for sem_at, known, away in ((1, two_down, -2), (3, plane > 0, -1), (2, plane < end, 1), (0, two_up, 2)):
        line_left(known, plane + away, line_send.at[sem_at])

    for source in sources:
        down, up = relays(source)
        line_left(down | up, 0, line_send.at[4 + source])

    for d in range(depth_count):
        for members, here in ((per - 1, depth == d), (per, depth != d)):
            both = takes_both(d, plane)
            for count, taken in ((2, both), (1, jnp.logical_not(both | takes_none(d, plane)))):
                @pl.when(here & taken)
                def _():
                    settle(other_in.at[:, pl.ds(0, members), :, pl.ds(0, count * sub)], other_send.at[d])

    settle(panel_in.at[:, 0, pl.ds(1, half_group - 1)], panel_send.at[0])
    settle(panel_in.at[:, 1], twin_send.at[0])
    settle(arrived.at[pl.ds(1, devices - 1)], last_send.at[0])
    settle(arrived.at[pl.ds(1, devices - 1)], last_recv.at[0])

    whole = own
    for t in range(1, devices):
        whole += arrived[t]
    out_ref[...] = whole


def half_shards(jacobian, gain_inverse, variance):
    rows, states = jacobian.shape
    depth_count = lax.axis_size("depth")
    blk_count = lax.axis_size("blk")
    devices = depth_count * blk_count
    per = blk_count // depth_count
    planes, group = depth_count, depth_count * per
    chunks = states // LANES
    sub = states // blk_count // LANES
    width = sub * LANES
    bf16, f32 = jnp.bfloat16, jnp.float32
    dma = pltpu.SemaphoreType.DMA
    quadratic = pl.pallas_call(
        functools.partial(half_kernel, depth_count, blk_count, rows),
        out_shape=pltpu.VMEM((1, LANES), f32),
        in_specs=[pl.BlockSpec(memory_space=pl.ANY)] * 2,
        out_specs=pl.BlockSpec(memory_space=pltpu.VMEM),
        scratch_shapes=[
            pltpu.VMEM((rows, states), bf16),
            pltpu.VMEM((rows * chunks, LANES), f32),
            pltpu.VMEM((planes, rows, chunks, LANES), bf16),
            pltpu.VMEM((planes, group, rows, per * sub, LANES), bf16),
            pltpu.VMEM((planes, 2, group // 2, rows, sub, LANES), bf16),
            pltpu.VMEM((3, devices * (rows * sub + 1), LANES), f32),
            pltpu.VMEM((2 * width, width), bf16),
            pltpu.VMEM((rows * devices, 2 * width), bf16),
            pltpu.VMEM((rows * devices, width), f32),
            pltpu.VMEM((rows, devices, LANES), f32),
            pltpu.VMEM((devices, 1, LANES), f32),
            pltpu.VMEM((devices, 1, LANES), f32),
            dma((3,)),
            dma((4 + planes,)),
            dma((planes, planes)),
            dma((depth_count,)),
            dma((planes,)),
            dma((1,)),
            dma((planes,)),
            dma((1,)),
            dma((planes,)),
            dma((1,)),
            dma((1,)),
        ],
        compiler_params=pltpu.CompilerParams(
            collective_id=0, has_side_effects=True, vmem_limit_bytes=60 * 1024 * 1024
        ),
    )(jacobian, gain_inverse)
    return variance - quadratic[0, :rows]


def solution(mesh):
    in_specs = (P(("depth", "blk"), None), P("depth", "blk"), P(("depth", "blk")))
    out_specs = P(("depth", "blk"))
    depth_count, blk_count = mesh.shape["depth"], mesh.shape["blk"]

    def shards(jacobian, gain_inverse, variance):
        width = gain_inverse.shape[1]
        fits = gain_inverse.size * gain_inverse.dtype.itemsize <= 16 * 1024 * 1024
        paired = 2 < depth_count <= 4 and depth_count % 2 == 0 and blk_count == 2 * depth_count
        if paired and width % (PACKED * LANES) == 0 and fits:
            return half_shards(jacobian, gain_inverse, variance)
        return plain_shards(jacobian, gain_inverse, variance)

    return jax.shard_map(shards, mesh=mesh, in_specs=in_specs, out_specs=out_specs, check_vma=False)
```

```python
import functools

import jax
import jax.numpy as jnp
from jax import lax
from jax.experimental import pallas as pl
from jax.experimental.pallas import tpu as pltpu
from jax.sharding import PartitionSpec as P

LANES = 128
SUBLANES = 8
PACKED = 16
MESH = pl.DeviceIdType.MESH


def exchange_kernel(depth_count, blk_count, slots, *refs):
    count = len(slots)
    sources, targets = refs[:count], refs[count : 2 * count]
    send_sem, recv_sem, own_sem = refs[2 * count :]
    devices = depth_count * blk_count
    me = lax.axis_index("depth") * blk_count + lax.axis_index("blk")

    def place(device):
        return {"depth": device // blk_count, "blk": lax.rem(device, blk_count)}

    def peer(step):
        return lax.rem(me + step, devices)

    def slot_of(kind, device):
        if kind == "depth":
            return device // blk_count
        if kind == "blk":
            return lax.rem(device, blk_count)
        return device

    def copy(which, step):
        device = peer(step)
        return pltpu.make_async_remote_copy(
            src_ref=sources[which].at[slot_of(slots[which], device)],
            dst_ref=targets[which].at[me],
            send_sem=send_sem.at[which, step],
            recv_sem=recv_sem.at[which, step],
            device_id=place(device),
            device_id_type=MESH,
        )

    barrier = pltpu.get_barrier_semaphore()

    @pl.loop(1, devices)
    def _(step):
        pl.semaphore_signal(barrier, inc=1, device_id=place(peer(step)), device_id_type=MESH)

    own = [
        pltpu.make_async_copy(sources[w].at[slot_of(slots[w], me)], targets[w].at[me], own_sem.at[w])
        for w in range(count)
    ]
    for w in range(count):
        own[w].start()
    pl.semaphore_wait(barrier, devices - 1)

    @pl.loop(1, devices)
    def _(step):
        for w in range(count):
            copy(w, step).start()

    for w in range(count):
        own[w].wait()

    @pl.loop(1, devices)
    def _(step):
        for w in range(count):
            copy(w, step).wait()


def exchange(slots, collective_id, *operands):
    depth_count = lax.axis_size("depth")
    blk_count = lax.axis_size("blk")
    devices = depth_count * blk_count
    count = len(slots)
    vmem = pl.BlockSpec(memory_space=pltpu.VMEM)
    return pl.pallas_call(
        functools.partial(exchange_kernel, depth_count, blk_count, slots),
        out_shape=[jax.ShapeDtypeStruct((devices,) + x.shape[1:], x.dtype) for x in operands],
        in_specs=[vmem] * count,
        out_specs=[vmem] * count,
        scratch_shapes=[
            pltpu.SemaphoreType.DMA((count, devices)),
            pltpu.SemaphoreType.DMA((count, devices)),
            pltpu.SemaphoreType.DMA((count,)),
        ],
        compiler_params=pltpu.CompilerParams(collective_id=collective_id, has_side_effects=True),
    )(*operands)


def sections(jacobian, parts):
    rows, states = jacobian.shape
    width = states // parts
    return jacobian.reshape(rows, parts, width // LANES, LANES).transpose(1, 0, 2, 3)


def plain_shards(jacobian, gain_inverse, variance):
    rows = jacobian.shape[0]
    depth_count = lax.axis_size("depth")
    blk_count = lax.axis_size("blk")
    devices = depth_count * blk_count
    left, right = exchange(
        ("depth", "blk"), 0, sections(jacobian, depth_count), sections(jacobian, blk_count)
    )
    left = left.reshape(devices * rows, -1)
    panel = right.reshape(devices * rows, -1)
    projected = jnp.dot(left, gain_inverse, preferred_element_type=jnp.float32)
    partial_sum = jnp.sum(projected * panel.astype(jnp.float32), axis=1)
    padded = jnp.pad(
        partial_sum.reshape(devices, 1, rows), ((0, 0), (0, SUBLANES - 1), (0, LANES - rows))
    )
    (gathered,) = exchange(("all",), 1, padded)
    quadratic = jnp.sum(gathered[:, 0, :rows], axis=0)
    return variance - quadratic


def half_kernel(
    depth_count, blk_count, rows, jac_ref, gain_ref, out_ref,
    own_raw, own_wide, lines, other_in, panel_in, wide, gain, left, projected, partial, outgoing, arrived,
    local_sem, line_send, line_recv, other_send, other_recv,
    panel_send, panel_recv, twin_send, twin_recv, last_send, last_recv, far_sem,
):
    per = blk_count // depth_count
    planes = depth_count
    group = depth_count * per
    half_group = group // 2
    devices = depth_count * blk_count
    states = jac_ref.shape[1]
    chunks = states // LANES
    sub = states // blk_count // LANES
    width = sub * LANES
    pitch = rows * sub + 1
    end = planes - 1
    depth = lax.axis_index("depth")
    blk = lax.axis_index("blk")
    plane = blk // per
    side = lax.rem(blk, per)
    spot = depth * per + side
    parity = lax.rem(depth, 2)
    twin = depth + 1 - 2 * parity
    seat = (depth // 2) * per + side
    on_diagonal = plane == depth

    def at_end(z):
        return (z == 0) | (z == end)

    def takes_none(d, z):
        return at_end(z) & jnp.logical_not(at_end(d))

    def takes_both(d, z):
        return at_end(d) & jnp.logical_not(at_end(z))

    idle = takes_none(depth, plane)
    double = takes_both(depth, plane)
    single = jnp.logical_not(idle | double)
    sources = [jnp.where(i < plane, plane - 1 - i, i + 1) for i in range(planes - 1)]

    def inside(z):
        return (z > 0) & (z < end)

    two_up = inside(plane + 2)
    two_down = inside(plane - 2)

    def near(d, s):
        return (d // 2 == depth // 2) | (s == side)

    def wrap(value, count):
        return jnp.where(value >= count, value - count, value)

    def other_section(d, z, s):
        return d * per + jnp.where(d < z, s, per - 1 - s)

    my_other = other_section(depth, plane, side)

    def section_of(source, section):
        return lines.at[source, :, pl.ds(pl.multiple_of(section * sub, sub), sub), :]

    def remote(src, dst, send_sem, recv_sem, d, b):
        return pltpu.make_async_remote_copy(
            src_ref=src, dst_ref=dst, send_sem=send_sem, recv_sem=recv_sem,
            device_id={"depth": d, "blk": b}, device_id_type=MESH,
        )

    def settle(ref, sem):
        pltpu.make_async_copy(ref, ref, sem).wait()

    jac_copy = pltpu.make_async_copy(jac_ref, own_raw, local_sem.at[0])
    jac_copy.start()
    gain_first = pltpu.make_async_copy(
        gain_ref.at[pl.ds(pl.multiple_of(jnp.where(double, 0, my_other - depth * per) * width, width), width), :],
        gain.at[pl.ds(0, width)], local_sem.at[1],
    )
    gain_second = pltpu.make_async_copy(
        gain_ref.at[pl.ds(pl.multiple_of(jnp.where(double, 1, side) * width, width), width), :],
        gain.at[pl.ds(width, width)], local_sem.at[2],
    )

    @pl.when(jnp.logical_not(idle))
    def _():
        gain_first.start()

    @pl.when(on_diagonal | double)
    def _():
        gain_second.start()

    barrier = pltpu.get_barrier_semaphore()

    def greet(d, b):
        pl.semaphore_signal(barrier, inc=1, device_id={"depth": d, "blk": b}, device_id_type=MESH)

    for s in range(1, group):
        member = wrap(spot + s, group)

        @pl.when(near(member // per, lax.rem(member, per)))
        def _():
            greet(member // per, plane * per + lax.rem(member, per))

    for away in (1, -1, 2, -2):
        known = (plane + away >= 0) & (plane + away <= end)
        if abs(away) == 2:
            known = known & inside(plane)

        @pl.when(known)
        def _():
            greet(depth, blk + away * per)

    jac_copy.wait()
    for c in range(chunks):
        own_wide[pl.ds(c, rows, stride=chunks), :] = own_raw[:, c * LANES : (c + 1) * LANES].astype(
            jnp.float32
        )
    for r in range(rows):
        lines[plane, r] = own_wide[r * chunks : (r + 1) * chunks, :].astype(jnp.bfloat16)

    heard = 2 * per - 1 + depth_count - 2
    for known in (plane > 0, plane < end, two_up, two_down):
        heard = heard + jnp.where(known, 1, 0)
    pl.semaphore_wait(barrier, heard)

    pl.semaphore_signal(
        far_sem, inc=1, device_id={"depth": depth, "blk": plane * per + per - 1 - side}, device_id_type=MESH
    )

    def along(source, part, target, send_sem):
        piece = lines.at[source, :, pl.ds(pl.multiple_of(part * (per * sub), per * sub), per * sub), :]
        return remote(piece, piece, send_sem, line_recv.at[source, part], depth, target * per + side)

    def nth_part(target, k):
        return jnp.where(2 * target < planes, wrap(planes - k, planes), wrap(end + k, planes))

    def part_count(target):
        return jnp.where(at_end(target), 2, planes)

    def send_line(target, sem_at, first, last):
        @pl.loop(first, last)
        def _(k):
            along(plane, nth_part(target, k), target, line_send.at[sem_at]).start()

    def seen_from(d, s):
        seen = spot - (d * per + s)
        return jnp.where(seen < 0, seen + group, seen)

    def to_other(source, d, s):
        return remote(
            section_of(source, other_section(d, plane, s)),
            other_in.at[source, seen_from(d, s), :, pl.ds(0, sub)],
            other_send.at[d], other_recv.at[source], d, plane * per + s,
        )

    def to_both(source, d, s):
        return remote(
            lines.at[source, :, pl.ds(pl.multiple_of(d * per * sub, per * sub), per * sub), :],
            other_in.at[source, seen_from(d, s)],
            other_send.at[d], other_recv.at[source], d, plane * per + s,
        )

    def to_panel(source, step):
        target = wrap(seat + step, half_group)
        s = lax.rem(target, per)
        return remote(
            section_of(source, plane * per + s), panel_in.at[source, 0, half_group - step],
            panel_send.at[0], panel_recv.at[source], (target // per) * 2 + parity, plane * per + s,
        )

    def own_to_twin(source):
        return remote(
            section_of(source, blk), panel_in.at[source, 1, 0],
            twin_send.at[0], twin_recv.at[source], twin, blk,
        )

    def pass_to_twin(source):
        return remote(
            panel_in.at[source, 0, pl.ds(1, half_group - 1)], panel_in.at[source, 1, pl.ds(1, half_group - 1)],
            twin_send.at[0], twin_recv.at[source], twin, blk,
        )

    def spread(source, part, which=None):
        for s in range(per):
            foreign = (part != depth) | (side != s)
            if which is not None:
                foreign = foreign & (near(part, s) == which)

            @pl.when(foreign & takes_both(part, plane))
            def _():
                to_both(source, part, s).start()

            @pl.when(foreign & (at_end(part) == at_end(plane)))
            def _():
                to_other(source, part, s).start()

    def spread_panel(source):
        for step in range(1, half_group):
            to_panel(source, step).start()
        own_to_twin(source).start()

    def forward_panel(source):
        settle(panel_in.at[source, 0, pl.ds(1, half_group - 1)], panel_recv.at[source])
        pass_to_twin(source).start()

    for sem_at, known, away in ((1, two_down, -2), (3, plane > 0, -1), (2, plane < end, 1), (0, two_up, 2)):
        @pl.when(known)
        def _():
            send_line(plane + away, sem_at, 0, 2)

    @pl.loop(0, planes)
    def _(k):
        spread(plane, nth_part(plane, k), True)

    pl.semaphore_wait(far_sem, 1)

    @pl.loop(0, planes)
    def _(k):
        spread(plane, nth_part(plane, k), False)

    spread_panel(plane)

    def relays(source):
        down = (plane == 1) & (source > 1)
        up = (plane == end - 1) & (source < end - 1)
        return down, up

    def send_rest():
        for sem_at, known, away in ((1, two_down, -2), (3, plane > 0, -1), (2, plane < end, 1), (0, two_up, 2)):
            @pl.when(known & jnp.logical_not(at_end(plane + away)))
            def _():
                send_line(plane + away, sem_at, 2, planes)

    def receive(source, k):
        down, up = relays(source)
        part = nth_part(plane, k)
        along(source, part, plane, line_send.at[0]).wait_recv()

        @pl.when((down | up) & (k < 2))
        def _():
            along(source, part, jnp.where(down, 0, end), line_send.at[4 + source]).start()

        spread(source, part)

    @pl.when(at_end(plane))
    def _():
        for n, source in enumerate(sources):
            @pl.loop(0, 2)
            def _(k):
                receive(source, k)
                if n == 0:
                    @pl.when(k == 0)
                    def _():
                        send_rest()

            if n:
                spread_panel(sources[n - 1])

        spread_panel(sources[-1])

    @pl.when(jnp.logical_not(at_end(plane)))
    def _():
        receive(sources[0], 0)
        send_rest()
        for source, first, stop in (
            (sources[0], 1, 2), (sources[1], 0, 2), (sources[2], 0, 2),
            (sources[0], 2, planes), (sources[1], 2, planes), (sources[2], 2, planes),
        ):
            @pl.loop(first, stop)
            def _(k):
                receive(source, k)

        for source in sources:
            spread_panel(source)

    def widen(index, slot, block):
        wide[index, pl.ds(slot * pitch, rows * sub), :] = block.reshape(rows * sub, LANES).astype(
            jnp.float32
        )

    def slot_of(source, d, s):
        return d * blk_count + source * per + s

    def collect_other(source):
        slot = slot_of(source, depth, side)

        def gather(first_section, count, indices):
            settle(other_in.at[source, pl.ds(1, group - 1), :, pl.ds(0, count * sub)], other_recv.at[source])
            for n, index in enumerate(indices):
                widen(index, slot, section_of(source, first_section + n)[...])

            @pl.loop(1, group)
            def _(k):
                member = wrap(spot + k, group)
                at = slot_of(source, member // per, lax.rem(member, per))
                for n, index in enumerate(indices):
                    widen(index, at, other_in[source, k, :, n * sub : (n + 1) * sub])

        @pl.when(single)
        def _():
            gather(my_other, 1, (0,))

        @pl.when(double)
        def _():
            gather(depth * per, 2, (0, 2))

    def collect_panel(source):
        widen(1, slot_of(source, depth, side), section_of(source, blk)[...])
        settle(panel_in.at[source, 1], twin_recv.at[source])

        @pl.loop(0, half_group)
        def _(k):
            at = wrap(seat + k, half_group)
            widen(1, slot_of(source, (at // per) * 2 + 1 - parity, lax.rem(at, per)), panel_in[source, 1, k])

            @pl.when(k > 0)
            def _():
                widen(1, slot_of(source, (at // per) * 2 + parity, lax.rem(at, per)), panel_in[source, 0, k])

    everything = [plane] + sources
    for source in everything:
        collect_other(source)

    def columns(index, c):
        return [wide[index, pl.ds(r * sub + c, devices, stride=pitch), :] for r in range(rows)]

    def narrow(first, source):
        for c in range(sub):
            for r, block in enumerate(columns(source, c)):
                left[r * devices : (r + 1) * devices, first + c * LANES : first + (c + 1) * LANES] = block.astype(
                    jnp.bfloat16
                )

    def dot(first, count, n=slice(0, width)):
        a = left[:, pl.ds(first, count)]
        return jnp.dot(a, gain[pl.ds(first, count), n], preferred_element_type=jnp.float32)

    half = width // 2
    halves = [slice(0, half), slice(half, width)]

    @pl.when(jnp.logical_not(idle))
    def _():
        narrow(0, 0)
        gain_first.wait()

    @pl.when(double)
    def _():
        narrow(width, 2)
        gain_second.wait()

    def multiply(n):
        at = halves[n]

        @pl.when(single & jnp.logical_not(on_diagonal))
        def _():
            projected[:, at] = dot(0, width, at)

        @pl.when(double)
        def _():
            projected[:, at] = dot(0, 2 * width, at)

        @pl.when(on_diagonal)
        def _():
            quarter = pl.multiple_of(jnp.where(side == 0, n, 1 - n) * half, half)
            projected[:, at] = dot(quarter, half, at)

    multiply(0)
    for source in everything:
        forward_panel(source)
    multiply(1)
    for source in everything:
        collect_panel(source)

    @pl.when(on_diagonal)
    def _():
        narrow(width, 1)
        gain_second.wait()
        projected[:, halves[0]] += 0.5 * dot(width, half, halves[0])
        projected[:, halves[1]] += dot(width, half, halves[1]) + 0.5 * dot(width + half, half, halves[1])

    @pl.when(idle)
    def _():
        partial[...] = jnp.zeros_like(partial)

    @pl.when(jnp.logical_not(idle))
    def _():
        total = [jnp.zeros((devices, LANES), jnp.float32) for _ in range(rows)]
        for c in range(sub):
            for r, panel in enumerate(columns(1, c)):
                total[r] += projected[r * devices : (r + 1) * devices, c * LANES : (c + 1) * LANES] * panel
        for r in range(rows):
            partial[r] = total[r]

    lane = lax.broadcasted_iota(jnp.int32, (devices, LANES), 1)
    packed = jnp.zeros((devices, LANES), jnp.float32)
    for r in range(rows):
        packed = jnp.where(lane == r, 2.0 * jnp.sum(partial[r], axis=1, keepdims=True), packed)
    for t in range(devices):
        outgoing[t] = packed[t : t + 1]

    def last(dd, db):
        d, b = depth ^ dd, blk ^ db
        return remote(
            outgoing.at[d * blk_count + b], arrived.at[dd * blk_count + db],
            last_send.at[0], last_recv.at[0], d, b,
        )

    for db in reversed(range(blk_count)):
        for dd in reversed(range(depth_count)):
            if dd or db:
                last(dd, db).start()

    own = outgoing[depth * blk_count + blk]

    def line_left(cond, target, sem):
        @pl.when(cond & at_end(target))
        def _():
            settle(lines.at[0, :, pl.ds(0, 2 * per * sub)], sem)

        @pl.when(cond & jnp.logical_not(at_end(target)))
        def _():
            settle(lines.at[0], sem)

    for sem_at, known, away in ((1, two_down, -2), (3, plane > 0, -1), (2, plane < end, 1), (0, two_up, 2)):
        line_left(known, plane + away, line_send.at[sem_at])

    for source in sources:
        down, up = relays(source)
        line_left(down | up, 0, line_send.at[4 + source])

    for d in range(depth_count):
        for members, here in ((per - 1, depth == d), (per, depth != d)):
            both = takes_both(d, plane)
            for count, taken in ((2, both), (1, jnp.logical_not(both | takes_none(d, plane)))):
                @pl.when(here & taken)
                def _():
                    settle(other_in.at[:, pl.ds(0, members), :, pl.ds(0, count * sub)], other_send.at[d])

    settle(panel_in.at[:, 0, pl.ds(1, half_group - 1)], panel_send.at[0])
    settle(panel_in.at[:, 1], twin_send.at[0])
    settle(arrived.at[pl.ds(1, devices - 1)], last_send.at[0])
    settle(arrived.at[pl.ds(1, devices - 1)], last_recv.at[0])

    whole = own
    for t in range(1, devices):
        whole += arrived[t]
    out_ref[...] = whole


def half_shards(jacobian, gain_inverse, variance):
    rows, states = jacobian.shape
    depth_count = lax.axis_size("depth")
    blk_count = lax.axis_size("blk")
    devices = depth_count * blk_count
    per = blk_count // depth_count
    planes, group = depth_count, depth_count * per
    chunks = states // LANES
    sub = states // blk_count // LANES
    width = sub * LANES
    bf16, f32 = jnp.bfloat16, jnp.float32
    dma = pltpu.SemaphoreType.DMA
    quadratic = pl.pallas_call(
        functools.partial(half_kernel, depth_count, blk_count, rows),
        out_shape=pltpu.VMEM((1, LANES), f32),
        in_specs=[pl.BlockSpec(memory_space=pl.ANY)] * 2,
        out_specs=pl.BlockSpec(memory_space=pltpu.VMEM),
        scratch_shapes=[
            pltpu.VMEM((rows, states), bf16),
            pltpu.VMEM((rows * chunks, LANES), f32),
            pltpu.VMEM((planes, rows, chunks, LANES), bf16),
            pltpu.VMEM((planes, group, rows, per * sub, LANES), bf16),
            pltpu.VMEM((planes, 2, group // 2, rows, sub, LANES), bf16),
            pltpu.VMEM((3, devices * (rows * sub + 1), LANES), f32),
            pltpu.VMEM((2 * width, width), bf16),
            pltpu.VMEM((rows * devices, 2 * width), bf16),
            pltpu.VMEM((rows * devices, width), f32),
            pltpu.VMEM((rows, devices, LANES), f32),
            pltpu.VMEM((devices, 1, LANES), f32),
            pltpu.VMEM((devices, 1, LANES), f32),
            dma((3,)),
            dma((4 + planes,)),
            dma((planes, planes)),
            dma((depth_count,)),
            dma((planes,)),
            dma((1,)),
            dma((planes,)),
            dma((1,)),
            dma((planes,)),
            dma((1,)),
            dma((1,)),
            pltpu.SemaphoreType.REGULAR,
        ],
        compiler_params=pltpu.CompilerParams(
            collective_id=0, has_side_effects=True, vmem_limit_bytes=60 * 1024 * 1024
        ),
    )(jacobian, gain_inverse)
    return variance - quadratic[0, :rows]


def solution(mesh):
    in_specs = (P(("depth", "blk"), None), P("depth", "blk"), P(("depth", "blk")))
    out_specs = P(("depth", "blk"))
    depth_count, blk_count = mesh.shape["depth"], mesh.shape["blk"]

    def shards(jacobian, gain_inverse, variance):
        width = gain_inverse.shape[1]
        fits = gain_inverse.size * gain_inverse.dtype.itemsize <= 16 * 1024 * 1024
        paired = 2 < depth_count <= 4 and depth_count % 2 == 0 and blk_count == 2 * depth_count
        if paired and width % (PACKED * LANES) == 0 and fits:
            return half_shards(jacobian, gain_inverse, variance)
        return plain_shards(jacobian, gain_inverse, variance)

    return jax.shard_map(shards, mesh=mesh, in_specs=in_specs, out_specs=out_specs, check_vma=False)
```
